128 devices in a mesh: data: 64 (over z, y, x), model: 2 (over core).
Axes of the slice: x: 4, y: 4, z: 4, core: 2. Of those that a mesh axis runs over, the one named last changes fastest.
Arguments:
- teacher_in: bfloat16 [512, 512, 1024], P('data', 'model')
- student_in: bfloat16 [512, 512, 384], P(('data', 'model'))
- teacher_gain: float32 [2, 1024], replicated
- teacher_up: bfloat16 [2, 1024, 4096], P(None, None, 'model')
- teacher_down: bfloat16 [2, 4096, 1024], P(None, 'model')
- student_gain: float32 [1, 384], replicated
- student_up: bfloat16 [1, 384, 1536], replicated
- student_down: bfloat16 [1, 1536, 384], replicated
- student_proj: bfloat16 [1, 1024, 384], replicated
Outputs:
- output 1: float32 [], replicated
- output 2: float32 [1, 384, 1536], replicated
- output 3: float32 [1, 1536, 384], replicated
- output 4: float32 [1, 384], replicated
- output 5: float32 [1, 1024, 384], replicated
All inputs are finite; a program needn't handle non-finite values.
Results may differ from the reference program's by a relative error of at most 0.00142751.
Values are sent between devices in bfloat16 or wider.
A program may use at most 1 GiB of HBM per device.

```python
import jax
import jax.numpy as jnp
from jax import lax

T_WIDTH = 1024
S_WIDTH = 384
T_LAYERS = 2
N_FEATS = 1
SEQ_LEN = 512
N_SEQS = 512
EPS = 1e-6


def setup_inputs(seed: int = 0) -> dict:
    keys = jax.random.split(jax.random.key(seed), 9)
    teach_ff = 4 * T_WIDTH
    stud_ff = 4 * S_WIDTH
    base = jax.random.normal(keys[0], (N_SEQS, SEQ_LEN, T_WIDTH), jnp.float32)
    noise = jax.random.normal(keys[1], (N_SEQS, SEQ_LEN, S_WIDTH), jnp.float32)
    return {
        "teacher_in": base.astype(jnp.bfloat16),
        "student_in": (0.8 * base[:, :, :S_WIDTH] + 0.6 * noise).astype(jnp.bfloat16),
        "teacher_gain": jax.random.uniform(keys[2], (T_LAYERS, T_WIDTH), jnp.float32, 0.25, 1.75),
        "teacher_up": (jax.random.normal(keys[3], (T_LAYERS, T_WIDTH, teach_ff), jnp.float32) * T_WIDTH ** -0.5).astype(jnp.bfloat16),
        "teacher_down": (jax.random.normal(keys[4], (T_LAYERS, teach_ff, T_WIDTH), jnp.float32) * teach_ff ** -0.5).astype(jnp.bfloat16),
        "student_gain": jax.random.uniform(keys[5], (N_FEATS, S_WIDTH), jnp.float32, 0.25, 1.75),
        "student_up": (jax.random.normal(keys[6], (N_FEATS, S_WIDTH, stud_ff), jnp.float32) * S_WIDTH ** -0.5).astype(jnp.bfloat16),
        "student_down": (jax.random.normal(keys[7], (N_FEATS, stud_ff, S_WIDTH), jnp.float32) * stud_ff ** -0.5).astype(jnp.bfloat16),
        "student_proj": (jax.random.normal(keys[8], (N_FEATS, T_WIDTH, S_WIDTH), jnp.float32) * T_WIDTH ** -0.5).astype(jnp.bfloat16),
    }


def rms_unit(values):
    return values * lax.rsqrt(jnp.mean(values * values, axis=-1, keepdims=True) + EPS)


def rms_back(values, grad_out):
    inv_rms = lax.rsqrt(jnp.mean(values * values, axis=-1, keepdims=True) + EPS)
    unit = values * inv_rms
    return inv_rms * (grad_out - unit * jnp.mean(grad_out * unit, axis=-1, keepdims=True))


def gelu_back(pre_act, grad_out):
    return jax.vjp(jax.nn.gelu, pre_act)[1](grad_out)[0]


def reference(teacher_in, student_in, teacher_gain, teacher_up, teacher_down, student_gain, student_up, student_down, student_proj):
    t_step = T_LAYERS // N_FEATS
    total = N_FEATS * N_SEQS * SEQ_LEN * S_WIDTH
    grad_scale = 2.0 / total
    teacher_groups = (
        teacher_gain.reshape(N_FEATS, t_step, T_WIDTH),
        teacher_up.reshape(N_FEATS, t_step, T_WIDTH, 4 * T_WIDTH),
        teacher_down.reshape(N_FEATS, t_step, 4 * T_WIDTH, T_WIDTH),
        student_proj,
    )

    def teacher_layer(hidden, layer):
        gain, w_up, w_down = layer
        act_in = (rms_unit(hidden.astype(jnp.float32)) * gain).astype(jnp.bfloat16)
        up_act = jax.nn.gelu(jnp.dot(act_in, w_up, preferred_element_type=jnp.float32)).astype(jnp.bfloat16)
        delta = jnp.dot(up_act, w_down, preferred_element_type=jnp.float32).astype(jnp.bfloat16)
        return (hidden.astype(jnp.float32) + delta.astype(jnp.float32)).astype(jnp.bfloat16), None

    def feature_group(hidden, group):
        gains, ups, downs, project = group
        hidden, _ = lax.scan(teacher_layer, hidden, (gains, ups, downs))
        target = jnp.dot(hidden, project, preferred_element_type=jnp.float32).astype(jnp.bfloat16)
        return hidden, (hidden, target)

    def student_block(state, block):
        gain, w_up, w_down, target = block
        normed = rms_unit(state.astype(jnp.float32))
        act_in = (normed * gain).astype(jnp.bfloat16)
        pre_act = jnp.dot(act_in, w_up, preferred_element_type=jnp.float32)
        up_act = jax.nn.gelu(pre_act).astype(jnp.bfloat16)
        new_state = (state.astype(jnp.float32) + jnp.dot(up_act, w_down, preferred_element_type=jnp.float32)).astype(jnp.bfloat16)
        error = target.astype(jnp.float32) - rms_unit(new_state.astype(jnp.float32))
        return new_state, (state, new_state, error)

    def student_back(d_res, saved):
        state, new_state, error, gain, w_up, w_down = saved
        d_res = d_res + rms_back(new_state.astype(jnp.float32), -grad_scale * error)
        normed = rms_unit(state.astype(jnp.float32))
        act_in = (normed * gain).astype(jnp.bfloat16)
        pre_act = jnp.dot(act_in, w_up, preferred_element_type=jnp.float32)
        up_act = jax.nn.gelu(pre_act).astype(jnp.bfloat16)
        d_out = d_res.astype(jnp.bfloat16)
        g_down = jnp.dot(up_act.T, d_out, preferred_element_type=jnp.float32)
        d_up = jnp.dot(d_out, w_down.T, preferred_element_type=jnp.float32)
        d_pre = gelu_back(pre_act, d_up).astype(jnp.bfloat16)
        g_up = jnp.dot(act_in.T, d_pre, preferred_element_type=jnp.float32)
        d_act = jnp.dot(d_pre, w_up.T, preferred_element_type=jnp.float32)
        g_gain = jnp.sum(d_act * normed, axis=0)
        d_res = d_res + rms_back(state.astype(jnp.float32), d_act * gain)
        return d_res, (g_up, g_down, g_gain)

    def proj_grad(pair):
        feature, error = pair
        return jnp.dot(feature.T, error.astype(jnp.bfloat16), preferred_element_type=jnp.float32)

    def one_sequence(carry, rows):
        teach_row, stud_row = rows
        _, (features, targets) = lax.scan(feature_group, teach_row, teacher_groups)
        _, saved = lax.scan(student_block, stud_row, (student_gain, student_up, student_down, targets))
        states, new_states, errors = saved
        _, (g_up, g_down, g_gain) = lax.scan(
            student_back,
            jnp.zeros((SEQ_LEN, S_WIDTH), jnp.float32),
            (states, new_states, errors, student_gain, student_up, student_down),
            reverse=True,
        )
        g_proj = grad_scale * lax.map(proj_grad, (features, errors))
        increment = (jnp.sum(errors * errors), g_up, g_down, g_gain, g_proj)
        return jax.tree.map(jnp.add, carry, increment), None

    start_sums = (
        jnp.zeros((), jnp.float32),
        jnp.zeros((N_FEATS, S_WIDTH, 4 * S_WIDTH), jnp.float32),
        jnp.zeros((N_FEATS, 4 * S_WIDTH, S_WIDTH), jnp.float32),
        jnp.zeros((N_FEATS, S_WIDTH), jnp.float32),
        jnp.zeros((N_FEATS, T_WIDTH, S_WIDTH), jnp.float32),
    )
    totals, _ = lax.scan(one_sequence, start_sums, (teacher_in, student_in))
    return (totals[0] / total, totals[1], totals[2], totals[3], totals[4])
```

```python
import functools

import jax
import jax.numpy as jnp
from jax import lax
from jax.experimental import pallas as pl
from jax.experimental.pallas import tpu as pltpu
from jax.sharding import PartitionSpec as P

EPS = 1e-6
F32 = jnp.float32
BF16 = jnp.bfloat16
MESH = pl.DeviceIdType.MESH
ROWS = 512
VMEM_MAX = 62 * 2**20
GELU_A = 0.7978845608028654
GELU_B = 0.044715


def rms_unit(values):
    return values * lax.rsqrt(jnp.mean(values * values, axis=-1, keepdims=True) + EPS)


def rms_back(values, grad_out):
    inv_rms = lax.rsqrt(jnp.mean(values * values, axis=-1, keepdims=True) + EPS)
    unit = values * inv_rms
    return inv_rms * (grad_out - unit * jnp.mean(grad_out * unit, axis=-1, keepdims=True))


def gelu(pre):
    half = 0.5 * pre
    return half + half * jnp.tanh(pre * (GELU_A + (GELU_A * GELU_B) * (pre * pre)))


def gelu_back(pre_act, grad_out):
    return jax.vjp(jax.nn.gelu, pre_act)[1](grad_out)[0]


def rows_of(blk):
    if isinstance(blk, int):
        return pl.ds(blk * ROWS, ROWS)
    return pl.ds(pl.multiple_of(blk * ROWS, ROWS), ROWS)


def up_half(a_v, w_v, blk, part):
    half = w_v.shape[1] // 2
    return jnp.dot(a_v[rows_of(blk), :], w_v[:, part * half : (part + 1) * half], preferred_element_type=F32)


def down_half(pre, w_v, part):
    half = w_v.shape[0] // 2
    return jnp.dot(gelu(pre).astype(BF16), w_v[part * half : (part + 1) * half, :], preferred_element_type=F32)


def partner():
    return {"model": 1 - lax.axis_index("model")}


def greet_partner():
    barrier = pltpu.get_barrier_semaphore()
    pl.semaphore_signal(barrier, inc=1, device_id=partner(), device_id_type=MESH)
    pl.semaphore_wait(barrier, 1)


def swap_copies(pairs, send_sem, recv_sem, parts):
    copies = []
    for idx, (src, dst) in enumerate(pairs):
        step = dst.shape[0] // parts
        for part in range(parts):
            span = pl.ds(part * step, step)
            slot = idx * parts + part
            copies.append(pltpu.make_async_remote_copy(
                src_ref=src.at[span], dst_ref=dst.at[span],
                send_sem=send_sem.at[slot], recv_sem=recv_sem.at[slot],
                device_id=partner(), device_id_type=MESH))
    return copies


def weight_loads(up, down, up_v, down_v, sems, base):
    half = up_v.shape[1] // 2
    lo, hi = pl.ds(0, half), pl.ds(half, half)
    pieces = [(up.at[:, lo], up_v.at[:, lo]), (up.at[:, hi], up_v.at[:, hi]), (down.at[lo, :], down_v.at[lo, :]), (down.at[hi, :], down_v.at[hi, :])]
    return [pltpu.make_async_copy(src, dst, sems.at[base + i]) for i, (src, dst) in enumerate(pieces)]


def first_kernel(n_blk, h_in, gain, up, down, acc_out, a_out, up_r, down_r, h_v, a_v, up_v, down_v, acc_v, p_v, h_sem, w_sem, o_sem, send_sem, recv_sem):
    loads = weight_loads(up.at[0], down.at[0], up_v, down_v, w_sem, 0)
    h_loads = [pltpu.make_async_copy(h_in.at[rows_of(b)], h_v.at[rows_of(b)], h_sem.at[b]) for b in range(n_blk)]
    h_loads[0].start()
    for load in loads:
        load.start()
    for b in range(1, n_blk):
        h_loads[b].start()
    greet_partner()
    sends = swap_copies([(up.at[0], up_r), (down.at[0], down_r)], send_sem, recv_sem, 4)
    for send in sends:
        send.start()

    def norm(b):
        a_v[rows_of(b), :] = (rms_unit(h_v[rows_of(b), :].astype(F32)) * gain[0:1, :]).astype(BF16)

    def outs(b):
        return [pltpu.make_async_copy(acc_v.at[rows_of(b)], acc_out.at[rows_of(b)], o_sem.at[b, 0]), pltpu.make_async_copy(a_v.at[rows_of(b)], a_out.at[rows_of(b)], o_sem.at[b, 1])]

    h_loads[0].wait()
    norm(0)
    loads[0].wait()
    p_v[0] = up_half(a_v, up_v, 0, 0)
    for load in loads[1:]:
        load.wait()
    for b in range(1, n_blk):
        h_loads[b].wait()

    def step(b, more):
        p_v[1] = up_half(a_v, up_v, b, 1)
        acc_v[rows_of(b), :] = down_half(p_v[0], down_v, 0)
        if more:
            norm(b + 1)
            p_v[0] = up_half(a_v, up_v, b + 1, 0)
        acc_v[rows_of(b), :] += down_half(p_v[1], down_v, 1)
        for out in outs(b):
            out.start()

    def loop_step(b, carry):
        step(b, True)
        return carry

    lax.fori_loop(0, n_blk - 1, loop_step, 0)
    step(n_blk - 1, False)
    for b in range(n_blk):
        for out in outs(b):
            out.wait()
    for send in sends:
        send.wait()


def middle_kernel(n_blk, h_in, a_in, acc_in, gain, up0, down0, up, down, h_out, acc_out, up_r, down_r, h_v, a_v, acc_v, up0_v, down0_v, up_v, down_v, p_v, h_sem, w_sem, o_sem, send_sem, recv_sem):
    loads = weight_loads(up0, down0, up0_v, down0_v, w_sem, 0)
    loads1 = weight_loads(up.at[1], down.at[1], up_v, down_v, w_sem, 4)
    blk_loads = []
    for b in range(n_blk):
        blk_loads.append([pltpu.make_async_copy(src.at[rows_of(b)], dst.at[rows_of(b)], h_sem.at[b, i]) for i, (src, dst) in enumerate([(a_in, a_v), (acc_in, acc_v), (h_in, h_v)])])
    blk_loads[0][0].start()
    loads[0].start()
    loads[1].start()
    loads[2].start()
    blk_loads[0][1].start()
    loads[3].start()
    blk_loads[0][2].start()
    for b in range(1, n_blk):
        for load in blk_loads[b]:
            load.start()
    for load in loads1:
        load.start()
    greet_partner()
    sends = swap_copies([(up.at[1], up_r), (down.at[1], down_r)], send_sem, recv_sem, 4)
    for send in sends:
        send.start()

    def finish(b):
        hid = (h_v[rows_of(b), :].astype(F32) + acc_v[rows_of(b), :].astype(BF16).astype(F32)).astype(BF16)
        h_v[rows_of(b), :] = hid
        a_v[rows_of(b), :] = (rms_unit(hid.astype(F32)) * gain[1:2, :]).astype(BF16)

    def outs(b):
        return [pltpu.make_async_copy(v.at[rows_of(b)], o.at[rows_of(b)], o_sem.at[b, i]) for i, (v, o) in enumerate([(h_v, h_out), (acc_v, acc_out)])]

    blk_loads[0][0].wait()
    loads[0].wait()
    p_v[0] = up_half(a_v, up0_v, 0, 0)
    for load in loads[1:]:
        load.wait()
    for b in range(n_blk):
        for load in blk_loads[b]:
            if not (b == 0 and load is blk_loads[0][0]):
                load.wait()
    p_v[1] = up_half(a_v, up0_v, 0, 1)
    acc_v[rows_of(0), :] += down_half(p_v[0], down0_v, 0)
    p_v[0] = up_half(a_v, up0_v, 1, 0)
    acc_v[rows_of(0), :] += down_half(p_v[1], down0_v, 1)
    for load in loads1:
        load.wait()

    def step(b, left):
        finish(b)
        if left >= 1:
            p_v[1] = up_half(a_v, up0_v, b + 1, 1)
            acc_v[rows_of(b + 1), :] += down_half(p_v[0], down0_v, 0)
        p_v[0] = up_half(a_v, up_v, b, 0)
        if left >= 1:
            acc_v[rows_of(b + 1), :] += down_half(p_v[1], down0_v, 1)
        p_v[1] = up_half(a_v, up_v, b, 1)
        acc_v[rows_of(b), :] = down_half(p_v[0], down_v, 0)
        if left >= 2:
            p_v[0] = up_half(a_v, up0_v, b + 2, 0)
        acc_v[rows_of(b), :] += down_half(p_v[1], down_v, 1)
        for out in outs(b):
            out.start()

    def loop_step(b, carry):
        step(b, 2)
        return carry

    lax.fori_loop(0, n_blk - 2, loop_step, 0)
    step(n_blk - 2, 1)
    step(n_blk - 1, 0)
    for b in range(n_blk):
        for out in outs(b):
            out.wait()
    for send in sends:
        send.wait()


def last_kernel(n_blk, h_in, acc_in, gain, up1, down1, f_out, h_v, a_v, acc_v, up_v, down_v, p_v, h_sem, w_sem, o_sem):
    loads = weight_loads(up1, down1, up_v, down_v, w_sem, 0)
    blk_loads = []
    for b in range(n_blk):
        blk_loads.append([pltpu.make_async_copy(src.at[rows_of(b)], dst.at[rows_of(b)], h_sem.at[b, i]) for i, (src, dst) in enumerate([(h_in, h_v), (acc_in, acc_v)])])
    blk_loads[0][0].start()
    for load in loads:
        load.start()
    for b in range(n_blk):
        for load in blk_loads[b]:
            if not (b == 0 and load is blk_loads[0][0]):
                load.start()

    def norm(b):
        a_v[rows_of(b), :] = (rms_unit(h_v[rows_of(b), :].astype(F32)) * gain[1:2, :]).astype(BF16)

    def out(b):
        return pltpu.make_async_copy(h_v.at[rows_of(b)], f_out.at[rows_of(b)], o_sem.at[b])

    blk_loads[0][0].wait()
    norm(0)
    loads[0].wait()
    p_v[0] = up_half(a_v, up_v, 0, 0)
    for load in loads[1:]:
        load.wait()
    for b in range(n_blk):
        for load in blk_loads[b]:
            if not (b == 0 and load is blk_loads[0][0]):
                load.wait()

    def step(b, more):
        p_v[1] = up_half(a_v, up_v, b, 1)
        acc_v[rows_of(b), :] += down_half(p_v[0], down_v, 0)
        if more:
            norm(b + 1)
            p_v[0] = up_half(a_v, up_v, b + 1, 0)
        acc = acc_v[rows_of(b), :] + down_half(p_v[1], down_v, 1)
        h_v[rows_of(b), :] = (h_v[rows_of(b), :].astype(F32) + acc.astype(BF16).astype(F32)).astype(BF16)
        out(b).start()

    def loop_step(b, carry):
        step(b, True)
        return carry

    lax.fori_loop(0, n_blk - 1, loop_step, 0)
    step(n_blk - 1, False)
    for b in range(n_blk):
        out(b).wait()


def any_specs(count):
    return [pl.BlockSpec(memory_space=pl.ANY)] * count


VM = pl.BlockSpec(memory_space=pltpu.VMEM)


def teacher(tokens, gain, up, down):
    n_tok, width = tokens.shape
    cols = up.shape[2]
    n_blk = n_tok // ROWS
    tok_bf = jax.ShapeDtypeStruct((n_tok, width), BF16)
    tok_f32 = jax.ShapeDtypeStruct((n_tok, width), F32)
    up_s, down_s = jax.ShapeDtypeStruct((width, cols), BF16), jax.ShapeDtypeStruct((cols, width), BF16)
    v_tok, v_acc = pltpu.VMEM((n_tok, width), BF16), pltpu.VMEM((n_tok, width), F32)
    v_up, v_down = pltpu.VMEM((width, cols), BF16), pltpu.VMEM((cols, width), BF16)
    v_p = pltpu.VMEM((2, ROWS, cols // 2), F32)
    dma = pltpu.SemaphoreType.DMA
    half_flops = 4 * n_tok * width * cols
    acc, a_first, up_r0, down_r0 = pl.pallas_call(
        functools.partial(first_kernel, n_blk),
        out_shape=(tok_f32, tok_bf, up_s, down_s),
        in_specs=[pl.BlockSpec(memory_space=pl.ANY), VM] + any_specs(2),
        out_specs=any_specs(4),
        scratch_shapes=[v_tok, v_tok, v_up, v_down, v_acc, v_p, dma((n_blk,)), dma((4,)), dma((n_blk, 2)), dma((8,)), dma((8,))],
        compiler_params=pltpu.CompilerParams(collective_id=0, has_side_effects=True, vmem_limit_bytes=VMEM_MAX),
        cost_estimate=pl.CostEstimate(flops=half_flops, bytes_accessed=2**25, transcendentals=0),
        name="teacher_first",
    )(tokens, gain, up, down)
    hid, acc, up_r1, down_r1 = pl.pallas_call(
        functools.partial(middle_kernel, n_blk),
        out_shape=(tok_bf, tok_f32, up_s, down_s),
        in_specs=any_specs(3) + [VM] + any_specs(4),
        out_specs=any_specs(4),
        scratch_shapes=[v_tok, v_tok, v_acc, v_up, v_down, v_up, v_down, v_p, dma((n_blk, 3)), dma((8,)), dma((n_blk, 2)), dma((8,)), dma((8,))],
        compiler_params=pltpu.CompilerParams(collective_id=1, has_side_effects=True, vmem_limit_bytes=VMEM_MAX),
        cost_estimate=pl.CostEstimate(flops=2 * half_flops, bytes_accessed=2**25, transcendentals=0),
        name="teacher_middle",
    )(tokens, a_first, acc, gain, up_r0, down_r0, up, down)
    return pl.pallas_call(
        functools.partial(last_kernel, n_blk),
        out_shape=tok_bf,
        in_specs=any_specs(2) + [VM] + any_specs(2),
        out_specs=pl.BlockSpec(memory_space=pl.ANY),
        scratch_shapes=[v_tok, v_tok, v_acc, v_up, v_down, v_p, dma((n_blk, 2)), dma((4,)), dma((n_blk,))],
        compiler_params=pltpu.CompilerParams(vmem_limit_bytes=VMEM_MAX),
        cost_estimate=pl.CostEstimate(flops=half_flops, bytes_accessed=2**25, transcendentals=0),
        name="teacher_last",
    )(hid, acc, gain, up_r1, down_r1)


def student_pass(student_in, targets, student_gain, student_up, student_down, grad_scale):
    n_feats = len(targets)
    state = student_in
    saved = []
    errors = []
    for feat_idx in range(n_feats):
        normed = rms_unit(state.astype(jnp.float32))
        act_in = (normed * student_gain[feat_idx]).astype(jnp.bfloat16)
        pre_act = jnp.einsum("sd,df->sf", act_in, student_up[feat_idx], preferred_element_type=jnp.float32)
        up_act = jax.nn.gelu(pre_act).astype(jnp.bfloat16)
        down_out = jnp.einsum("sf,fd->sd", up_act, student_down[feat_idx], preferred_element_type=jnp.float32)
        new_state = (state.astype(jnp.float32) + down_out).astype(jnp.bfloat16)
        errors.append(targets[feat_idx].astype(jnp.float32) - rms_unit(new_state.astype(jnp.float32)))
        saved.append((state, normed, act_in, pre_act, up_act, new_state))
        state = new_state
    loss_sum = sum(jnp.sum(error * error) for error in errors)
    d_res = jnp.zeros(student_in.shape, jnp.float32)
    grads_up = []
    grads_down = []
    grads_gain = []
    for feat_idx in reversed(range(n_feats)):
        state, normed, act_in, pre_act, up_act, new_state = saved[feat_idx]
        d_res = d_res + rms_back(new_state.astype(jnp.float32), -grad_scale * errors[feat_idx])
        d_out = d_res.astype(jnp.bfloat16)
        grads_down.append(jnp.einsum("sf,sd->fd", up_act, d_out, preferred_element_type=jnp.float32))
        d_up = jnp.einsum("sd,fd->sf", d_out, student_down[feat_idx], preferred_element_type=jnp.float32)
        d_pre = gelu_back(pre_act, d_up).astype(jnp.bfloat16)
        grads_up.append(jnp.einsum("sd,sf->df", act_in, d_pre, preferred_element_type=jnp.float32))
        d_act = jnp.einsum("sf,df->sd", d_pre, student_up[feat_idx], preferred_element_type=jnp.float32)
        grads_gain.append(jnp.sum(d_act * normed, axis=0))
        if feat_idx > 0:
            d_res = d_res + rms_back(state.astype(jnp.float32), d_act * student_gain[feat_idx])
    return loss_sum, errors, jnp.stack(grads_up[::-1]), jnp.stack(grads_down[::-1]), jnp.stack(grads_gain[::-1])


def student_rows(student_in):
    seqs, length, width = student_in.shape
    core = lax.axis_index("model")
    half = length // 2
    keep = lax.dynamic_slice_in_dim(student_in, core * half, half, axis=1)
    give = lax.dynamic_slice_in_dim(student_in, (1 - core) * half, half, axis=1)
    got = lax.ppermute(give, "model", [(0, 1), (1, 0)])
    low = jnp.where(core == 0, keep, got)
    high = jnp.where(core == 0, got, keep)
    return jnp.concatenate([low, high], axis=0).reshape(2 * seqs * half, width)


def solution(mesh):
    dev_count = mesh.shape["data"] * mesh.shape["model"]
    all_axes = ("data", "model")

    def body(teacher_in, student_in, teacher_gain, teacher_up, teacher_down, student_gain, student_up, student_down, student_proj):
        seq_rows, seq_len, s_width = student_in.shape
        total = seq_rows * dev_count * seq_len * s_width
        grad_scale = 2.0 / total
        t_width = teacher_in.shape[2]
        feat = teacher(teacher_in.reshape(-1, t_width), teacher_gain, teacher_up, teacher_down)
        rows = student_rows(student_in)
        target = jnp.dot(feat, student_proj[0], preferred_element_type=F32).astype(BF16)
        loss_sum, errors, grad_up, grad_down, grad_gain = student_pass(rows, [target], student_gain, student_up, student_down, grad_scale)
        grad_proj = grad_scale * jnp.einsum("sd,se->de", feat, errors[0].astype(BF16), preferred_element_type=F32)
        totals = lax.psum((loss_sum, grad_up, grad_down, grad_gain, grad_proj[None]), all_axes)
        return (totals[0] / total, totals[1], totals[2], totals[3], totals[4])

    return jax.shard_map(
        body,
        mesh=mesh,
        in_specs=(
            P("data", "model", None),
            P(("data", "model"), None, None),
            P(),
            P(None, None, "model"),
            P(None, "model", None),
            P(),
            P(),
            P(),
            P(),
        ),
        out_specs=(P(), P(), P(), P(), P()),
        check_vma=False,
    )
```

```python
import functools

import jax
import jax.numpy as jnp
from jax import lax
from jax.experimental import pallas as pl
from jax.experimental.pallas import tpu as pltpu
from jax.sharding import PartitionSpec as P

EPS = 1e-6
F32 = jnp.float32
BF16 = jnp.bfloat16
MESH = pl.DeviceIdType.MESH
ROWS = 512
VMEM_MAX = 62 * 2**20
GELU_A = 0.7978845608028654
GELU_B = 0.044715


def rms_unit(values):
    return values * lax.rsqrt(jnp.mean(values * values, axis=-1, keepdims=True) + EPS)


def rms_back(values, grad_out):
    inv_rms = lax.rsqrt(jnp.mean(values * values, axis=-1, keepdims=True) + EPS)
    unit = values * inv_rms
    return inv_rms * (grad_out - unit * jnp.mean(grad_out * unit, axis=-1, keepdims=True))


def gelu(pre):
    half = 0.5 * pre
    return half + half * jnp.tanh(pre * (GELU_A + (GELU_A * GELU_B) * (pre * pre)))


def rows_of(blk):
    if isinstance(blk, int):
        return pl.ds(blk * ROWS, ROWS)
    return pl.ds(pl.multiple_of(blk * ROWS, ROWS), ROWS)


def up_half(a_v, w_v, blk, part):
    half = w_v.shape[1] // 2
    return jnp.dot(a_v[rows_of(blk), :], w_v[:, part * half : (part + 1) * half], preferred_element_type=F32)


def down_half(pre, w_v, part):
    half = w_v.shape[0] // 2
    return jnp.dot(gelu(pre).astype(BF16), w_v[part * half : (part + 1) * half, :], preferred_element_type=F32)


def partner():
    return {"model": 1 - lax.axis_index("model")}


def greet_partner():
    barrier = pltpu.get_barrier_semaphore()
    pl.semaphore_signal(barrier, inc=1, device_id=partner(), device_id_type=MESH)
    pl.semaphore_wait(barrier, 1)


def swap_copies(pairs, send_sem, recv_sem, parts):
    copies = []
    for idx, (src, dst) in enumerate(pairs):
        step = dst.shape[0] // parts
        for part in range(parts):
            span = pl.ds(part * step, step)
            slot = idx * parts + part
            copies.append(pltpu.make_async_remote_copy(
                src_ref=src.at[span], dst_ref=dst.at[span],
                send_sem=send_sem.at[slot], recv_sem=recv_sem.at[slot],
                device_id=partner(), device_id_type=MESH))
    return copies


def weight_loads(up, down, up_v, down_v, sems, base):
    half = up_v.shape[1] // 2
    lo, hi = pl.ds(0, half), pl.ds(half, half)
    pieces = [(up.at[:, lo], up_v.at[:, lo]), (up.at[:, hi], up_v.at[:, hi]), (down.at[lo, :], down_v.at[lo, :]), (down.at[hi, :], down_v.at[hi, :])]
    return [pltpu.make_async_copy(src, dst, sems.at[base + i]) for i, (src, dst) in enumerate(pieces)]


def first_kernel(n_blk, h_in, gain, up, down, stud, acc_out, a_out, up_r, down_r, stud_r, h_v, a_v, up_v, down_v, acc_v, p_v, h_sem, w_sem, o_sem, send_sem, recv_sem):
    loads = weight_loads(up.at[0], down.at[0], up_v, down_v, w_sem, 0)
    h_loads = [pltpu.make_async_copy(h_in.at[rows_of(b)], h_v.at[rows_of(b)], h_sem.at[b]) for b in range(n_blk)]
    h_loads[0].start()
    for load in loads:
        load.start()
    for b in range(1, n_blk):
        h_loads[b].start()
    greet_partner()
    sends = swap_copies([(up.at[0], up_r), (down.at[0], down_r)], send_sem, recv_sem, 4)
    half_len = stud.shape[1] // 2
    give = pl.ds(pl.multiple_of((1 - lax.axis_index("model")) * half_len, half_len), half_len)
    sends.append(pltpu.make_async_remote_copy(src_ref=stud.at[:, give], dst_ref=stud_r, send_sem=send_sem.at[8], recv_sem=recv_sem.at[8], device_id=partner(), device_id_type=MESH))
    for send in sends:
        send.start()

    def norm(b):
        a_v[rows_of(b), :] = (rms_unit(h_v[rows_of(b), :].astype(F32)) * gain[0:1, :]).astype(BF16)

    def outs(b):
        return [pltpu.make_async_copy(acc_v.at[rows_of(b)], acc_out.at[rows_of(b)], o_sem.at[b, 0]), pltpu.make_async_copy(a_v.at[rows_of(b)], a_out.at[rows_of(b)], o_sem.at[b, 1])]

    h_loads[0].wait()
    norm(0)
    loads[0].wait()
    p_v[0] = up_half(a_v, up_v, 0, 0)
    for load in loads[1:]:
        load.wait()
    for b in range(1, n_blk):
        h_loads[b].wait()

    def step(b, more):
        p_v[1] = up_half(a_v, up_v, b, 1)
        acc_v[rows_of(b), :] = down_half(p_v[0], down_v, 0)
        if more:
            norm(b + 1)
            p_v[0] = up_half(a_v, up_v, b + 1, 0)
        acc_v[rows_of(b), :] += down_half(p_v[1], down_v, 1)
        for out in outs(b):
            out.start()

    def loop_step(b, carry):
        step(b, True)
        return carry

    lax.fori_loop(0, n_blk - 1, loop_step, 0)
    step(n_blk - 1, False)
    for b in range(n_blk):
        for out in outs(b):
            out.wait()
    for send in sends:
        send.wait()


def middle_kernel(n_blk, h_in, a_in, acc_in, gain, up0, down0, up, down, h_out, acc_out, up_r, down_r, h_v, a_v, acc_v, up0_v, down0_v, up_v, down_v, p_v, h_sem, w_sem, o_sem, send_sem, recv_sem):
    loads = weight_loads(up0, down0, up0_v, down0_v, w_sem, 0)
    loads1 = weight_loads(up.at[1], down.at[1], up_v, down_v, w_sem, 4)
    blk_loads = []
    for b in range(n_blk):
        blk_loads.append([pltpu.make_async_copy(src.at[rows_of(b)], dst.at[rows_of(b)], h_sem.at[b, i]) for i, (src, dst) in enumerate([(a_in, a_v), (acc_in, acc_v), (h_in, h_v)])])
    blk_loads[0][0].start()
    loads[0].start()
    loads[1].start()
    loads[2].start()
    blk_loads[0][1].start()
    loads[3].start()
    blk_loads[0][2].start()
    for b in range(1, n_blk):
        for load in blk_loads[b]:
            load.start()
    for load in loads1:
        load.start()
    greet_partner()
    sends = swap_copies([(up.at[1], up_r), (down.at[1], down_r)], send_sem, recv_sem, 4)
    for send in sends:
        send.start()

    def finish(b):
        hid = (h_v[rows_of(b), :].astype(F32) + acc_v[rows_of(b), :].astype(BF16).astype(F32)).astype(BF16)
        h_v[rows_of(b), :] = hid
        a_v[rows_of(b), :] = (rms_unit(hid.astype(F32)) * gain[1:2, :]).astype(BF16)

    def outs(b):
        return [pltpu.make_async_copy(v.at[rows_of(b)], o.at[rows_of(b)], o_sem.at[b, i]) for i, (v, o) in enumerate([(h_v, h_out), (acc_v, acc_out)])]

    blk_loads[0][0].wait()
    loads[0].wait()
    p_v[0] = up_half(a_v, up0_v, 0, 0)
    for load in loads[1:]:
        load.wait()
    for b in range(n_blk):
        for load in blk_loads[b]:
            if not (b == 0 and load is blk_loads[0][0]):
                load.wait()
    p_v[1] = up_half(a_v, up0_v, 0, 1)
    acc_v[rows_of(0), :] += down_half(p_v[0], down0_v, 0)
    p_v[0] = up_half(a_v, up0_v, 1, 0)
    acc_v[rows_of(0), :] += down_half(p_v[1], down0_v, 1)
    for load in loads1:
        load.wait()

    def step(b, left):
        finish(b)
        if left >= 1:
            p_v[1] = up_half(a_v, up0_v, b + 1, 1)
            acc_v[rows_of(b + 1), :] += down_half(p_v[0], down0_v, 0)
        p_v[0] = up_half(a_v, up_v, b, 0)
        if left >= 1:
            acc_v[rows_of(b + 1), :] += down_half(p_v[1], down0_v, 1)
        p_v[1] = up_half(a_v, up_v, b, 1)
        acc_v[rows_of(b), :] = down_half(p_v[0], down_v, 0)
        if left >= 2:
            p_v[0] = up_half(a_v, up0_v, b + 2, 0)
        acc_v[rows_of(b), :] += down_half(p_v[1], down_v, 1)
        for out in outs(b):
            out.start()

    def loop_step(b, carry):
        step(b, 2)
        return carry

    lax.fori_loop(0, n_blk - 2, loop_step, 0)
    step(n_blk - 2, 1)
    step(n_blk - 1, 0)
    for b in range(n_blk):
        for out in outs(b):
            out.wait()
    for send in sends:
        send.wait()


def last_kernel(n_blk, h_in, acc_in, gain, up1, down1, f_out, h_v, a_v, acc_v, up_v, down_v, p_v, h_sem, w_sem, o_sem):
    loads = weight_loads(up1, down1, up_v, down_v, w_sem, 0)
    blk_loads = []
    for b in range(n_blk):
        blk_loads.append([pltpu.make_async_copy(src.at[rows_of(b)], dst.at[rows_of(b)], h_sem.at[b, i]) for i, (src, dst) in enumerate([(h_in, h_v), (acc_in, acc_v)])])
    blk_loads[0][0].start()
    for load in loads:
        load.start()
    for b in range(n_blk):
        for load in blk_loads[b]:
            if not (b == 0 and load is blk_loads[0][0]):
                load.start()

    def norm(b):
        a_v[rows_of(b), :] = (rms_unit(h_v[rows_of(b), :].astype(F32)) * gain[1:2, :]).astype(BF16)

    def out(b):
        return pltpu.make_async_copy(h_v.at[rows_of(b)], f_out.at[rows_of(b)], o_sem.at[b])

    blk_loads[0][0].wait()
    norm(0)
    loads[0].wait()
    p_v[0] = up_half(a_v, up_v, 0, 0)
    for load in loads[1:]:
        load.wait()
    for b in range(n_blk):
        for load in blk_loads[b]:
            if not (b == 0 and load is blk_loads[0][0]):
                load.wait()

    def step(b, more):
        p_v[1] = up_half(a_v, up_v, b, 1)
        acc_v[rows_of(b), :] += down_half(p_v[0], down_v, 0)
        if more:
            norm(b + 1)
            p_v[0] = up_half(a_v, up_v, b + 1, 0)
        acc = acc_v[rows_of(b), :] + down_half(p_v[1], down_v, 1)
        h_v[rows_of(b), :] = (h_v[rows_of(b), :].astype(F32) + acc.astype(BF16).astype(F32)).astype(BF16)
        out(b).start()

    def loop_step(b, carry):
        step(b, True)
        return carry

    lax.fori_loop(0, n_blk - 1, loop_step, 0)
    step(n_blk - 1, False)
    for b in range(n_blk):
        out(b).wait()


def any_specs(count):
    return [pl.BlockSpec(memory_space=pl.ANY)] * count


VM = pl.BlockSpec(memory_space=pltpu.VMEM)


def teacher(tokens, gain, up, down, stud):
    seqs, length, s_width = stud.shape
    stud_s = jax.ShapeDtypeStruct((seqs, length // 2, s_width), BF16)
    n_tok, width = tokens.shape
    cols = up.shape[2]
    n_blk = n_tok // ROWS
    tok_bf = jax.ShapeDtypeStruct((n_tok, width), BF16)
    tok_f32 = jax.ShapeDtypeStruct((n_tok, width), F32)
    up_s, down_s = jax.ShapeDtypeStruct((width, cols), BF16), jax.ShapeDtypeStruct((cols, width), BF16)
    v_tok, v_acc = pltpu.VMEM((n_tok, width), BF16), pltpu.VMEM((n_tok, width), F32)
    v_up, v_down = pltpu.VMEM((width, cols), BF16), pltpu.VMEM((cols, width), BF16)
    v_p = pltpu.VMEM((2, ROWS, cols // 2), F32)
    dma = pltpu.SemaphoreType.DMA
    half_flops = 4 * n_tok * width * cols
    acc, a_first, up_r0, down_r0, stud_r = pl.pallas_call(
        functools.partial(first_kernel, n_blk),
        out_shape=(tok_f32, tok_bf, up_s, down_s, stud_s),
        in_specs=[pl.BlockSpec(memory_space=pl.ANY), VM] + any_specs(3),
        out_specs=any_specs(5),
        scratch_shapes=[v_tok, v_tok, v_up, v_down, v_acc, v_p, dma((n_blk,)), dma((4,)), dma((n_blk, 2)), dma((9,)), dma((9,))],
        compiler_params=pltpu.CompilerParams(collective_id=0, has_side_effects=True, vmem_limit_bytes=VMEM_MAX),
        cost_estimate=pl.CostEstimate(flops=half_flops, bytes_accessed=2**25, transcendentals=0),
        name="teacher_first",
    )(tokens, gain, up, down, stud)
    hid, acc, up_r1, down_r1 = pl.pallas_call(
        functools.partial(middle_kernel, n_blk),
        out_shape=(tok_bf, tok_f32, up_s, down_s),
        in_specs=any_specs(3) + [VM] + any_specs(4),
        out_specs=any_specs(4),
        scratch_shapes=[v_tok, v_tok, v_acc, v_up, v_down, v_up, v_down, v_p, dma((n_blk, 3)), dma((8,)), dma((n_blk, 2)), dma((8,)), dma((8,))],
        compiler_params=pltpu.CompilerParams(collective_id=1, has_side_effects=True, vmem_limit_bytes=VMEM_MAX),
        cost_estimate=pl.CostEstimate(flops=2 * half_flops, bytes_accessed=2**25, transcendentals=0),
        name="teacher_middle",
    )(tokens, a_first, acc, gain, up_r0, down_r0, up, down)
    feat = pl.pallas_call(
        functools.partial(last_kernel, n_blk),
        out_shape=tok_bf,
        in_specs=any_specs(2) + [VM] + any_specs(2),
        out_specs=pl.BlockSpec(memory_space=pl.ANY),
        scratch_shapes=[v_tok, v_tok, v_acc, v_up, v_down, v_p, dma((n_blk, 2)), dma((4,)), dma((n_blk,))],
        compiler_params=pltpu.CompilerParams(vmem_limit_bytes=VMEM_MAX),
        cost_estimate=pl.CostEstimate(flops=half_flops, bytes_accessed=2**25, transcendentals=0),
        name="teacher_last",
    )(hid, acc, gain, up_r1, down_r1)
    return feat, stud_r


PART = 128
SIDE = PART // 2
RING = 4
STRIDES = (1, RING, RING * RING)
OTHERS = (2, 1, 3)


def gelu_pair(pre):
    sq = pre * pre
    tanh = jnp.tanh(pre * (GELU_A + (GELU_A * GELU_B) * sq))
    cdf = 0.5 + 0.5 * tanh
    slope = cdf + (0.5 * pre) * ((1.0 - tanh * tanh) * (GELU_A + (3.0 * GELU_A * GELU_B) * sq))
    return pre * cdf, slope


def dot_rows(lhs, rhs):
    return lax.dot_general(lhs, rhs, (((0,), (0,)), ((), ())), preferred_element_type=F32)


def dot_cols(lhs, rhs):
    return lax.dot_general(lhs, rhs, (((1,), (1,)), ((), ())), preferred_element_type=F32)


def axis_coord(stride):
    return (lax.axis_index("data") // stride) % RING


def axis_peer(stride, offset):
    coord = axis_coord(stride)
    return {"data": lax.axis_index("data") + (((coord + offset) % RING) - coord) * stride}


def span(index, size):
    return pl.ds(pl.multiple_of(index * size, size), size)


class PartSum:
    def __init__(self, ops, credit, g_v, bufs, part, first_col, n_cols):
        self.sender, self.credit, self.g_v, self.part = ops, credit, g_v, part
        self.core_v, self.fwd_v, self.fsum_v, self.near_v, self.p2_v, self.r2_v, self.slots_v = [buf.at[part] for buf in bufs]
        self.wide = n_cols // RING
        self.first_col, self.n_cols = first_col, n_cols
        self.axes = [STRIDES[(part + i) % len(STRIDES)] for i in range(len(STRIDES))]
        self.coords = [axis_coord(stride) for stride in self.axes]
        self.row0 = part * PART + lax.axis_index("model") * SIDE
        self.up, self.down = axis_peer(self.axes[0], 1), axis_peer(self.axes[0], RING - 1)
        self.cols = pl.ds(first_col, n_cols)

    def rows(self, offset, size):
        return pl.ds(pl.multiple_of(self.row0 + offset, size), size)

    def lanes(self, shift):
        return span((self.coords[0] + shift) % RING, self.wide)

    def out(self, offset, size, shift):
        lanes = pl.ds(pl.multiple_of(self.first_col + ((self.coords[0] + shift) % RING) * self.wide, 128), self.wide)
        return self.g_v.at[self.rows(offset, size), lanes]

    def core_send(self):
        away = pl.ds(pl.multiple_of(self.part * PART + (1 - lax.axis_index("model")) * SIDE, SIDE), SIDE)
        self.core = self.sender(self.g_v.at[away, self.cols], self.core_v, partner(), True)

    def ring_start(self):
        self.core.wait()
        pl.semaphore_signal(self.credit, inc=1, device_id=partner(), device_id_type=MESH)
        self.core_v[...] = self.core_v[...] + self.g_v[self.rows(0, SIDE), self.cols]
        half = SIDE // 2
        lo, hi = pl.ds(0, half), pl.ds(half, half)
        self.fwd = [self.sender(self.core_v.at[lo, self.lanes(2)], self.fwd_v.at[0], self.up), self.sender(self.core_v.at[hi, self.lanes(2)], self.fwd_v.at[1], self.down)]
        self.near = [self.sender(self.core_v.at[hi, self.lanes(1)], self.near_v.at[0, hi], self.up), self.sender(self.core_v.at[lo, self.lanes(3)], self.near_v.at[1, lo], self.down)]

    def ring_forward(self):
        half = SIDE // 2
        for which, shift, dev in ((0, 1, self.up), (1, 3, self.down)):
            rows = pl.ds(which * half, half)
            self.fwd[which].wait_recv()
            self.fsum_v[which] = self.fwd_v[which] + self.core_v[rows, self.lanes(shift)]
            self.near.append(self.sender(self.fsum_v.at[which], self.near_v.at[which, rows], dev))

    def second_start(self):
        for copy in self.near:
            copy.wait_recv()
        self.p2_v[...] = self.core_v[:, self.lanes(0)] + (self.near_v[0] + self.near_v[1])
        size = SIDE // RING
        self.r2 = [self.sender(self.p2_v.at[span((self.coords[1] + off) % RING, size)], self.r2_v.at[off - 1], axis_peer(self.axes[1], off)) for off in OTHERS]

    def third_start(self):
        for copy in self.r2:
            copy.wait_recv()
        slot = self.slots_v.at[self.coords[2]]
        slot[...] = (self.p2_v[span(self.coords[1], SIDE // RING), :] + self.r2_v[1]) + (self.r2_v[0] + self.r2_v[2])
        self.r3 = [self.sender(slot, slot, axis_peer(self.axes[2], off)) for off in OTHERS]

    def back_second(self):
        for copy in self.r3:
            copy.wait_recv()
        size = SIDE // RING
        block = self.out(self.coords[1] * size, size, 0)
        block[...] = (self.slots_v[0] + self.slots_v[1]) + (self.slots_v[2] + self.slots_v[3])
        self.b2 = [self.sender(block, block, axis_peer(self.axes[1], off)) for off in OTHERS]

    def back_first(self):
        for copy in self.b2:
            copy.wait_recv()
        half = SIDE // 2
        lo, hi = self.out(0, half, 0), self.out(half, half, 0)
        self.early = [self.sender(lo, lo, self.up), self.sender(hi, hi, self.down)]
        self.late = [self.sender(hi, hi, self.up), self.sender(lo, lo, self.down)]
        self.cross = []
        pl.semaphore_wait(self.credit, 1)
        self.give(0)

    def give(self, shift):
        block = self.out(0, SIDE, shift)
        self.cross.append(self.sender(block, block, partner()))

    def back_forward(self):
        half = SIDE // 2
        self.far = []
        for which, shift, dev in ((0, 3, self.up), (1, 1, self.down)):
            self.early[which].wait_recv()
            block = self.out(which * half, half, shift)
            self.far.append(self.sender(block, block, dev))

    def back_core(self):
        for which, shift in ((0, 3), (1, 1)):
            self.late[which].wait_recv()
            self.give(shift)

    def back_last(self):
        for copy in self.far:
            copy.wait_recv()
        self.give(2)

    def finish(self):
        for copy in self.cross:
            copy.wait_recv()


STAGES = ("core_send", "ring_start", "ring_forward", "second_start", "third_start", "back_second", "back_first", "back_forward", "back_core", "back_last", "finish")


class SmallSum:
    def __init__(self, sender, small_v, slots_v):
        self.sender, self.small_v, self.slots_v, self.level = sender, small_v, slots_v, 0

    def send(self):
        level = self.level
        coord = lax.axis_index("model") if level == 0 else axis_coord(STRIDES[level - 1])
        slots = self.slots_v.at[level]
        slots[coord] = self.small_v[level]
        peers = [partner()] if level == 0 else [axis_peer(STRIDES[level - 1], off) for off in OTHERS]
        self.copies = [self.sender(self.small_v.at[level], slots.at[coord], dev) for dev in peers]

    def add(self):
        for copy in self.copies:
            copy.wait_recv()
        slots = self.slots_v.at[self.level]
        total = slots[0] + slots[1]
        if self.level > 0:
            total = total + (slots[2] + slots[3])
        self.level += 1
        self.small_v[self.level] = total


def student_kernel(n_blk, grad_scale, f_in, stud, stud_r, s_gain, s_up, s_down, s_proj, g_out, small_out, f_v, s_v, su_v, sd_v, sp_v, u_v, slope_v, act_v, d_v, e_v, g_v, small_v, slots_v, *rest):
    bufs_a, bufs_b = rest[:7], rest[7:14]
    f_sem, s_sem, o_sem, send_sem, recv_sem, credit = rest[14:]
    core = lax.axis_index("model")
    seqs, half_len, s_width = stud_r.shape
    f_width = s_up.shape[2]
    t_width = s_proj.shape[1]
    keep = span(core, half_len)
    f_loads = [pltpu.make_async_copy(f_in.at[rows_of(b)], f_v.at[rows_of(b)], f_sem.at[b]) for b in range(n_blk)]
    pairs = [(stud.at[:, keep], s_v.at[pl.ds(core * seqs, seqs)]), (stud_r, s_v.at[pl.ds((1 - core) * seqs, seqs)]), (s_up.at[0], su_v), (s_proj.at[0], sp_v), (s_down.at[0], sd_v)]
    s_loads = [pltpu.make_async_copy(src, dst, s_sem.at[i]) for i, (src, dst) in enumerate(pairs)]
    for load in s_loads + f_loads:
        load.start()
    barrier = pltpu.get_barrier_semaphore()
    peers = [partner()] + [axis_peer(stride, off) for stride in STRIDES for off in OTHERS]
    for peer in peers:
        pl.semaphore_signal(barrier, inc=1, device_id=peer, device_id_type=MESH)
    pl.semaphore_wait(barrier, len(peers))
    started = []

    def sender(src, dst, dev, waited=False):
        slot = len(started)
        copy = pltpu.make_async_remote_copy(src_ref=src, dst_ref=dst, send_sem=send_sem.at[slot], recv_sem=recv_sem.at[slot], device_id=dev, device_id_type=MESH)
        copy.start()
        started.append(None if waited else copy)
        return copy

    parts = range(s_width // PART)
    group_a = [PartSum(sender, credit.at[0, k], g_v, bufs_a, k, f_width, f_width + t_width) for k in parts]
    group_b = [PartSum(sender, credit.at[1, k], g_v, bufs_b, k, 0, f_width) for k in parts]
    small = SmallSum(sender, small_v, slots_v)

    def run(group, num):
        for part in group:
            getattr(part, STAGES[num])()

    small_v[0] = jnp.zeros(small_v.shape[1:], F32)
    for load in s_loads + f_loads:
        load.wait()

    def state_of(b):
        n_seq = ROWS // half_len
        return s_v[pl.ds(b * n_seq, n_seq)].reshape(ROWS, s_width).astype(F32)

    def forward(b, carry):
        state = state_of(b)
        target = jnp.dot(f_v[rows_of(b), :], sp_v[...], preferred_element_type=F32).astype(BF16)
        act = (rms_unit(state) * s_gain[...]).astype(BF16)
        act_v[rows_of(b), :] = act
        up_act, slope = gelu_pair(jnp.dot(act, su_v[...], preferred_element_type=F32))
        up_act = up_act.astype(BF16)
        slope_v[rows_of(b), :] = slope
        u_v[rows_of(b), :] = up_act
        new_state = (state + jnp.dot(up_act, sd_v[...], preferred_element_type=F32)).astype(BF16).astype(F32)
        error = target.astype(F32) - rms_unit(new_state)
        small_v[0, 1:2, 0:s_width] += jnp.sum(error * error, axis=0, keepdims=True)
        e_v[rows_of(b), :] = error.astype(BF16)
        d_v[rows_of(b), :] = rms_back(new_state, -grad_scale * error).astype(BF16)
        return carry

    def backward(b, carry):
        u_v[rows_of(b), :] = (slope_v[rows_of(b), :] * dot_cols(d_v[rows_of(b), :], sd_v[...])).astype(BF16)
        return carry

    def gain_sum(b, carry):
        d_act = dot_cols(u_v[rows_of(b), :], su_v[...])
        small_v[0, 0:1, 0:s_width] += jnp.sum(d_act * rms_unit(state_of(b)), axis=0, keepdims=True)
        return carry

    lax.fori_loop(0, n_blk, forward, 0)
    g_v[:, 2 * f_width : 2 * f_width + t_width] = grad_scale * dot_rows(e_v[...], f_v[...])
    g_v[:, f_width : 2 * f_width] = dot_rows(d_v[...], u_v[...])
    run(group_a, 0)
    lax.fori_loop(0, n_blk, backward, 0)
    run(group_a, 1)
    g_v[:, 0:f_width] = dot_rows(act_v[...], u_v[...])
    run(group_b, 0)
    run(group_a, 2)
    lax.fori_loop(0, n_blk // 2, gain_sum, 0)
    run(group_b, 1)
    lax.fori_loop(n_blk // 2, n_blk, gain_sum, 0)
    small_v[0, 2:3, 0:PART] = jnp.broadcast_to(jnp.sum(small_v[0, 1:2, 0:s_width], axis=1, keepdims=True), (1, PART))
    small.send()
    for num in range(2, len(STAGES)):
        run(group_b, num)
        if num + 1 < len(STAGES):
            run(group_a, num + 1)
        if small.level <= len(STRIDES):
            small.add()
            if small.level <= len(STRIDES):
                small.send()
            else:
                small_out[...] = small_v[small.level]
    out = pltpu.make_async_copy(g_v, g_out, o_sem.at[0])
    out.start()
    out.wait()
    for copy in started:
        if copy is not None:
            copy.wait_send()


def sum_bufs(parts, n_cols):
    wide, vmem = n_cols // RING, pltpu.VMEM
    half, quarter = SIDE // 2, SIDE // RING
    shapes = [(SIDE, n_cols), (2, half, wide), (2, half, wide), (2, SIDE, wide), (SIDE, wide), (len(OTHERS), quarter, wide), (RING, quarter, wide)]
    return [vmem((parts,) + shape, F32) for shape in shapes]


def student_sums(feat, stud, stud_r, s_gain, s_up, s_down, s_proj, grad_scale):
    n_tok, width = feat.shape
    n_blk = n_tok // ROWS
    seqs, half_len, s_width = stud_r.shape
    f_width = s_up.shape[2]
    n_cols = 2 * f_width + width
    parts = s_width // PART
    dma = pltpu.SemaphoreType.DMA
    vmem = pltpu.VMEM
    v_act = vmem((n_tok, s_width), BF16)
    small = (8, s_width)
    n_copies = 200
    return pl.pallas_call(
        functools.partial(student_kernel, n_blk, grad_scale),
        out_shape=(jax.ShapeDtypeStruct((s_width, n_cols), F32), jax.ShapeDtypeStruct(small, F32)),
        in_specs=any_specs(3) + [VM] + any_specs(3),
        out_specs=(pl.BlockSpec(memory_space=pl.ANY), VM),
        scratch_shapes=[
            vmem((n_tok, width), BF16), vmem((n_tok // half_len, half_len, s_width), BF16), vmem((s_width, f_width), BF16), vmem((f_width, s_width), BF16), vmem((width, s_width), BF16),
            vmem((n_tok, f_width), BF16), vmem((n_tok, f_width), F32), v_act, v_act, v_act, vmem((s_width, n_cols), F32), vmem((5,) + small, F32), vmem((4, 4) + small, F32)]
        + sum_bufs(parts, f_width + width) + sum_bufs(parts, f_width)
        + [dma((n_blk,)), dma((5,)), dma((1,)), dma((n_copies,)), dma((n_copies,)), pltpu.SemaphoreType.REGULAR((2, parts))],
        compiler_params=pltpu.CompilerParams(collective_id=2, has_side_effects=True, vmem_limit_bytes=VMEM_MAX),
        cost_estimate=pl.CostEstimate(flops=2**34, bytes_accessed=2**24, transcendentals=0),
        name="student_sums",
    )(feat, stud, stud_r, s_gain, s_up, s_down, s_proj)


def solution(mesh):
    dev_count = mesh.shape["data"] * mesh.shape["model"]

    def body(teacher_in, student_in, teacher_gain, teacher_up, teacher_down, student_gain, student_up, student_down, student_proj):
        seq_rows, seq_len, s_width = student_in.shape
        total = seq_rows * dev_count * seq_len * s_width
        grad_scale = 2.0 / total
        t_width = teacher_in.shape[2]
        f_width = student_up.shape[2]
        feat, stud_r = teacher(teacher_in.reshape(-1, t_width), teacher_gain, teacher_up, teacher_down, student_in)
        grads, small = student_sums(feat, student_in, stud_r, student_gain, student_up, student_down, student_proj, grad_scale)
        grad_up = grads[:, 0:f_width]
        grad_down = grads[:, f_width : 2 * f_width].T
        grad_proj = grads[:, 2 * f_width :].T
        return (small[2, 0] / total, grad_up[None], grad_down[None], small[0:1, 0:s_width], grad_proj[None])

    return jax.shard_map(
        body,
        mesh=mesh,
        in_specs=(
            P("data", "model", None),
            P(("data", "model"), None, None),
            P(),
            P(None, None, "model"),
            P(None, "model", None),
            P(),
            P(),
            P(),
            P(),
        ),
        out_specs=(P(), P(), P(), P(), P()),
        check_vma=False,
    )
```

```python
import functools

import jax
import jax.numpy as jnp
from jax import lax
from jax.experimental import pallas as pl
from jax.experimental.pallas import tpu as pltpu
from jax.sharding import PartitionSpec as P

EPS = 1e-6
F32 = jnp.float32
BF16 = jnp.bfloat16
MESH = pl.DeviceIdType.MESH
ROWS = 512
VMEM_MAX = 62 * 2**20
GELU_A = 0.7978845608028654
GELU_B = 0.044715


def rms_unit(values):
    return values * lax.rsqrt(jnp.mean(values * values, axis=-1, keepdims=True) + EPS)


def rms_back(values, grad_out):
    inv_rms = lax.rsqrt(jnp.mean(values * values, axis=-1, keepdims=True) + EPS)
    unit = values * inv_rms
    return inv_rms * (grad_out - unit * jnp.mean(grad_out * unit, axis=-1, keepdims=True))


def gelu(pre):
    half = 0.5 * pre
    return half + half * jnp.tanh(pre * (GELU_A + (GELU_A * GELU_B) * (pre * pre)))


def rows_of(blk):
    return pl.ds(pl.multiple_of(blk * ROWS, ROWS), ROWS)


def partner():
    return {"model": 1 - lax.axis_index("model")}


def greet_partner():
    barrier = pltpu.get_barrier_semaphore()
    pl.semaphore_signal(barrier, inc=1, device_id=partner(), device_id_type=MESH)
    pl.semaphore_wait(barrier, 1)


def teacher_kernel(n_blk, h_in, gain, up, down, stud, f_out, stud_r, h_v, a_v, acc_v, p_v, up_v, down_v, h_sem, w_sem, o_sem, send_sem, recv_sem):
    half = up_v.shape[2] // 2
    n_tok = h_v.shape[0]

    def blk(b):
        return pl.ds(pl.multiple_of(b * ROWS, ROWS), ROWS)

    h_loads = [pltpu.make_async_copy(h_in.at[blk(b)], h_v.at[blk(b)], h_sem.at[b]) for b in range(n_blk)]
    w_loads = [
        [
            pltpu.make_async_copy(up.at[layer, :, pl.ds(part * half, half)], up_v.at[2 * layer, :, pl.ds(part * half, half)], w_sem.at[layer, part])
            for part in range(2)
        ]
        + [pltpu.make_async_copy(down.at[layer], down_v.at[2 * layer], w_sem.at[layer, 2])]
        for layer in range(2)
    ]
    for load in h_loads + w_loads[0]:
        load.start()
    greet_partner()
    swaps = []
    for layer in range(2):
        group = []
        for idx, (src, dst) in enumerate([(up, up_v), (down, down_v)]):
            step = src.shape[1] // 4
            for piece in range(4):
                rows = pl.ds(piece * step, step)
                sems = (layer, idx, piece)
                group.append(pltpu.make_async_remote_copy(
                    src_ref=src.at[layer, rows], dst_ref=dst.at[2 * layer + 1, rows],
                    send_sem=send_sem.at[sems], recv_sem=recv_sem.at[sems], device_id=partner(), device_id_type=MESH))
        swaps.append(group)
    for copy in swaps[0]:
        copy.start()
    for load in w_loads[1]:
        load.start()
    half_len = stud.shape[1] // 2
    give = pl.ds(pl.multiple_of((1 - lax.axis_index("model")) * half_len, half_len), half_len)
    last = (2, 0, 0)
    swaps[1].append(pltpu.make_async_remote_copy(src_ref=stud.at[:, give], dst_ref=stud_r, send_sem=send_sem.at[last], recv_sem=recv_sem.at[last], device_id=partner(), device_id_type=MESH))
    for copy in swaps[1]:
        copy.start()

    def norm(b, layer):
        a_v[blk(b), :] = (rms_unit(h_v[blk(b), :].astype(F32)) * gain[pl.ds(layer, 1), :]).astype(BF16)

    def up_part(unit, part):
        cols = pl.ds(part * half, half)
        p_v[part] = jnp.dot(a_v[blk(unit % n_blk), :], up_v[unit // n_blk, :, cols], preferred_element_type=F32)

    def down_part(unit, part):
        acc_v[blk(unit % n_blk), :] += jnp.dot(gelu(p_v[part]).astype(BF16), down_v[unit // n_blk, pl.ds(part * half, half), :], preferred_element_type=F32)

    def finish(b, layer):
        h_v[blk(b), :] = (h_v[blk(b), :].astype(F32) + acc_v[blk(b), :].astype(BF16).astype(F32)).astype(BF16)
        acc_v[blk(b), :] = jnp.zeros((ROWS, acc_v.shape[1]), F32)
        norm(b, jnp.minimum(layer + 1, 1))

    def out(b):
        return pltpu.make_async_copy(h_v.at[blk(b)], f_out.at[blk(b)], o_sem.at[b])

    def clear(i, carry):
        acc_v[pl.ds(pl.multiple_of(i * 64, 64), 64), :] = jnp.zeros((64, acc_v.shape[1]), F32)
        return carry

    lax.fori_loop(0, n_tok // 64, clear, 0)
    h_loads[0].wait()
    norm(0, 0)
    w_loads[0][0].wait()
    up_part(0, 0)
    for load in h_loads[1:]:
        load.wait()

    def norm_step(b, carry):
        norm(b, 0)
        return carry

    lax.fori_loop(1, n_blk, norm_step, 0)
    for load in w_loads[0][1:]:
        load.wait()
    end = 4 * n_blk

    def arrive(unit, at, copies, remote):
        @pl.when(unit == at)
        def _():
            for copy in copies:
                if remote:
                    copy.wait_recv()
                else:
                    copy.wait()

    def layer_step(layer, carry):
        def plain(unit, inner):
            arrive(unit, n_blk - 1, swaps[0], True)
            arrive(unit, 3 * n_blk - 1, swaps[1], True)
            up_part(unit, 1)
            down_part(unit, 0)
            up_part(unit + 1, 0)
            down_part(unit, 1)
            return inner

        def closing(unit, inner):
            arrive(unit, 2 * n_blk - 1, w_loads[1], False)
            done = unit - (n_blk + 1) - 2 * n_blk * layer
            up_part(unit, 1)
            down_part(unit, 0)
            finish(done, layer)
            up_part(jnp.minimum(unit + 1, end - 1), 0)
            down_part(unit, 1)

            @pl.when(layer == 1)
            def _():
                out(done).start()

            return inner

        lax.fori_loop((2 * n_blk + 1) * layer, (n_blk + 1) + 2 * n_blk * layer, plain, 0)
        lax.fori_loop((n_blk + 1) + 2 * n_blk * layer, (2 * n_blk + 1) + (2 * n_blk - 1) * layer, closing, 0)
        return carry

    lax.fori_loop(0, 2, layer_step, 0)
    b_last = n_blk - 1
    h_v[blk(b_last), :] = (h_v[blk(b_last), :].astype(F32) + acc_v[blk(b_last), :].astype(BF16).astype(F32)).astype(BF16)
    out(b_last).start()
    for b in range(n_blk):
        out(b).wait()
    for group in swaps:
        for copy in group:
            copy.wait_send()


def any_specs(count):
    return [pl.BlockSpec(memory_space=pl.ANY)] * count


VM = pl.BlockSpec(memory_space=pltpu.VMEM)


def teacher(tokens, gain, up, down, stud):
    n_tok, width = tokens.shape
    cols = up.shape[2]
    n_blk = n_tok // ROWS
    seqs, length, s_width = stud.shape
    dma, vmem = pltpu.SemaphoreType.DMA, pltpu.VMEM
    v_tok = vmem((n_tok, width), BF16)
    return pl.pallas_call(
        functools.partial(teacher_kernel, n_blk),
        out_shape=(jax.ShapeDtypeStruct((n_tok, width), BF16), jax.ShapeDtypeStruct((seqs, length // 2, s_width), BF16)),
        in_specs=[pl.BlockSpec(memory_space=pl.ANY), VM] + any_specs(3),
        out_specs=any_specs(2),
        scratch_shapes=[v_tok, v_tok, vmem((n_tok, width), F32), vmem((2, ROWS, cols // 2), F32), vmem((4, width, cols), BF16), vmem((4, cols, width), BF16),
                        dma((n_blk,)), dma((2, 3)), dma((n_blk,)), dma((3, 2, 4)), dma((3, 2, 4))],
        compiler_params=pltpu.CompilerParams(collective_id=0, has_side_effects=True, vmem_limit_bytes=VMEM_MAX),
        cost_estimate=pl.CostEstimate(flops=16 * n_tok * width * cols, bytes_accessed=2**25, transcendentals=0),
        name="teacher",
    )(tokens, gain, up, down, stud)


PART = 128
SIDE = PART // 2
RING = 4
STRIDES = (1, RING, RING * RING)
OTHERS = (2, 1, 3)


def gelu_pair(pre):
    sq = pre * pre
    tanh = jnp.tanh(pre * (GELU_A + (GELU_A * GELU_B) * sq))
    cdf = 0.5 + 0.5 * tanh
    slope = cdf + (0.5 * pre) * ((1.0 - tanh * tanh) * (GELU_A + (3.0 * GELU_A * GELU_B) * sq))
    return pre * cdf, slope


def dot_rows(lhs, rhs):
    return lax.dot_general(lhs, rhs, (((0,), (0,)), ((), ())), preferred_element_type=F32)


def dot_cols(lhs, rhs):
    return lax.dot_general(lhs, rhs, (((1,), (1,)), ((), ())), preferred_element_type=F32)


def axis_coord(stride):
    return (lax.axis_index("data") // stride) % RING


def axis_peer(stride, offset):
    coord = axis_coord(stride)
    return {"data": lax.axis_index("data") + (((coord + offset) % RING) - coord) * stride}


def span(index, size):
    return pl.ds(pl.multiple_of(index * size, size), size)


class PartSum:
    def __init__(self, ops, credit, g_v, bufs, part, first_col, n_cols):
        self.sender, self.credit, self.g_v, self.part = ops, credit, g_v, part
        self.core_v, self.fwd_v, self.fsum_v, self.near_v, self.p2_v, self.r2_v, self.slots_v = [buf.at[part] for buf in bufs]
        self.wide = n_cols // RING
        self.first_col, self.n_cols = first_col, n_cols
        self.axes = [STRIDES[(part + i) % len(STRIDES)] for i in range(len(STRIDES))]
        self.coords = [axis_coord(stride) for stride in self.axes]
        self.row0 = part * PART + lax.axis_index("model") * SIDE
        self.up, self.down = axis_peer(self.axes[0], 1), axis_peer(self.axes[0], RING - 1)
        self.cols = pl.ds(first_col, n_cols)

    def rows(self, offset, size):
        return pl.ds(pl.multiple_of(self.row0 + offset, size), size)

    def lanes(self, shift):
        return span((self.coords[0] + shift) % RING, self.wide)

    def out(self, offset, size, shift):
        lanes = pl.ds(pl.multiple_of(self.first_col + ((self.coords[0] + shift) % RING) * self.wide, 128), self.wide)
        return self.g_v.at[self.rows(offset, size), lanes]

    def core_send(self):
        away = pl.ds(pl.multiple_of(self.part * PART + (1 - lax.axis_index("model")) * SIDE, SIDE), SIDE)
        self.core = self.sender(self.g_v.at[away, self.cols], self.core_v, partner(), True)

    def ring_start(self):
        self.core.wait()
        pl.semaphore_signal(self.credit, inc=1, device_id=partner(), device_id_type=MESH)
        self.core_v[...] = self.core_v[...] + self.g_v[self.rows(0, SIDE), self.cols]
        half = SIDE // 2
        lo, hi = pl.ds(0, half), pl.ds(half, half)
        self.fwd = [self.sender(self.core_v.at[lo, self.lanes(2)], self.fwd_v.at[0], self.up), self.sender(self.core_v.at[hi, self.lanes(2)], self.fwd_v.at[1], self.down)]
        self.near = [self.sender(self.core_v.at[hi, self.lanes(1)], self.near_v.at[0, hi], self.up), self.sender(self.core_v.at[lo, self.lanes(3)], self.near_v.at[1, lo], self.down)]

    def ring_forward(self):
        half = SIDE // 2
        for which, shift, dev in ((0, 1, self.up), (1, 3, self.down)):
            rows = pl.ds(which * half, half)
            self.fwd[which].wait_recv()
            self.fsum_v[which] = self.fwd_v[which] + self.core_v[rows, self.lanes(shift)]
            self.near.append(self.sender(self.fsum_v.at[which], self.near_v.at[which, rows], dev))

    def second_start(self):
        for copy in self.near:
            copy.wait_recv()
        self.p2_v[...] = self.core_v[:, self.lanes(0)] + (self.near_v[0] + self.near_v[1])
        size = SIDE // RING
        self.r2 = [self.sender(self.p2_v.at[span((self.coords[1] + off) % RING, size)], self.r2_v.at[off - 1], axis_peer(self.axes[1], off)) for off in OTHERS]

    def third_start(self):
        for copy in self.r2:
            copy.wait_recv()
        slot = self.slots_v.at[self.coords[2]]
        slot[...] = (self.p2_v[span(self.coords[1], SIDE // RING), :] + self.r2_v[1]) + (self.r2_v[0] + self.r2_v[2])
        self.r3 = [self.sender(slot, slot, axis_peer(self.axes[2], off)) for off in OTHERS]

    def back_second(self):
        for copy in self.r3:
            copy.wait_recv()
        size = SIDE // RING
        block = self.out(self.coords[1] * size, size, 0)
        block[...] = (self.slots_v[0] + self.slots_v[1]) + (self.slots_v[2] + self.slots_v[3])
        self.b2 = [self.sender(block, block, axis_peer(self.axes[1], off)) for off in OTHERS]

    def back_first(self):
        for copy in self.b2:
            copy.wait_recv()
        half = SIDE // 2
        lo, hi = self.out(0, half, 0), self.out(half, half, 0)
        self.early = [self.sender(lo, lo, self.up), self.sender(hi, hi, self.down)]
        self.late = [self.sender(hi, hi, self.up), self.sender(lo, lo, self.down)]
        self.cross = []
        pl.semaphore_wait(self.credit, 1)
        self.give(0)

    def give(self, shift):
        block = self.out(0, SIDE, shift)
        self.cross.append(self.sender(block, block, partner()))

    def back_forward(self):
        half = SIDE // 2
        self.far = []
        for which, shift, dev in ((0, 3, self.up), (1, 1, self.down)):
            self.early[which].wait_recv()
            block = self.out(which * half, half, shift)
            self.far.append(self.sender(block, block, dev))

    def back_core(self):
        for which, shift in ((0, 3), (1, 1)):
            self.late[which].wait_recv()
            self.give(shift)

    def back_last(self):
        for copy in self.far:
            copy.wait_recv()
        self.give(2)

    def finish(self):
        for copy in self.cross:
            copy.wait_recv()


STAGES = ("core_send", "ring_start", "ring_forward", "second_start", "third_start", "back_second", "back_first", "back_forward", "back_core", "back_last", "finish")


class SmallSum:
    def __init__(self, sender, small_v, slots_v):
        self.sender, self.small_v, self.slots_v, self.level = sender, small_v, slots_v, 0

    def send(self):
        level = self.level
        coord = lax.axis_index("model") if level == 0 else axis_coord(STRIDES[level - 1])
        slots = self.slots_v.at[level]
        slots[coord] = self.small_v[level]
        peers = [partner()] if level == 0 else [axis_peer(STRIDES[level - 1], off) for off in OTHERS]
        self.copies = [self.sender(self.small_v.at[level], slots.at[coord], dev) for dev in peers]

    def add(self):
        for copy in self.copies:
            copy.wait_recv()
        slots = self.slots_v.at[self.level]
        total = slots[0] + slots[1]
        if self.level > 0:
            total = total + (slots[2] + slots[3])
        self.level += 1
        self.small_v[self.level] = total


def student_kernel(n_blk, grad_scale, f_in, stud, stud_r, s_gain, s_up, s_down, s_proj, up_out, down_out, proj_out, small_out, f_v, s_v, su_v, sd_v, sp_v, u_v, slope_v, act_v, d_v, e_v, g_v, small_v, slots_v, *rest):
    bufs_a, bufs_b = rest[:7], rest[7:14]
    f_sem, s_sem, o_sem, send_sem, recv_sem, credit = rest[14:]
    core = lax.axis_index("model")
    seqs, half_len, s_width = stud_r.shape
    f_width = s_up.shape[2]
    t_width = s_proj.shape[1]
    keep = span(core, half_len)
    f_loads = [pltpu.make_async_copy(f_in.at[rows_of(b)], f_v.at[rows_of(b)], f_sem.at[b]) for b in range(n_blk)]
    pairs = [(stud.at[:, keep], s_v.at[pl.ds(core * seqs, seqs)]), (stud_r, s_v.at[pl.ds((1 - core) * seqs, seqs)]), (s_up.at[0], su_v), (s_proj.at[0], sp_v), (s_down.at[0], sd_v)]
    s_loads = [pltpu.make_async_copy(src, dst, s_sem.at[i]) for i, (src, dst) in enumerate(pairs)]
    for load in s_loads + f_loads:
        load.start()
    barrier = pltpu.get_barrier_semaphore()
    peers = [partner()] + [axis_peer(stride, off) for stride in STRIDES for off in OTHERS]
    for peer in peers:
        pl.semaphore_signal(barrier, inc=1, device_id=peer, device_id_type=MESH)
    pl.semaphore_wait(barrier, len(peers))
    started = []

    def sender(src, dst, dev, waited=False):
        slot = len(started)
        copy = pltpu.make_async_remote_copy(src_ref=src, dst_ref=dst, send_sem=send_sem.at[slot], recv_sem=recv_sem.at[slot], device_id=dev, device_id_type=MESH)
        copy.start()
        started.append(None if waited else copy)
        return copy

    parts = range(s_width // PART)
    group_a = [PartSum(sender, credit.at[0, k], g_v, bufs_a, k, f_width, f_width + t_width) for k in parts]
    group_b = [PartSum(sender, credit.at[1, k], g_v, bufs_b, k, 0, f_width) for k in parts]
    small = SmallSum(sender, small_v, slots_v)

    def run(group, num):
        for part in group:
            getattr(part, STAGES[num])()

    small_v[0] = jnp.zeros(small_v.shape[1:], F32)
    for load in s_loads + f_loads:
        load.wait()

    def state_of(b):
        n_seq = ROWS // half_len
        return s_v[pl.ds(b * n_seq, n_seq)].reshape(ROWS, s_width).astype(F32)

    def forward(b, carry):
        state = state_of(b)
        target = jnp.dot(f_v[rows_of(b), :], sp_v[...], preferred_element_type=F32).astype(BF16)
        act = (rms_unit(state) * s_gain[...]).astype(BF16)
        act_v[rows_of(b), :] = act
        up_act, slope = gelu_pair(jnp.dot(act, su_v[...], preferred_element_type=F32))
        up_act = up_act.astype(BF16)
        slope_v[rows_of(b), :] = slope
        u_v[rows_of(b), :] = up_act
        new_state = (state + jnp.dot(up_act, sd_v[...], preferred_element_type=F32)).astype(BF16).astype(F32)
        error = target.astype(F32) - rms_unit(new_state)
        small_v[0, 1:2, 0:s_width] += jnp.sum(error * error, axis=0, keepdims=True)
        e_v[rows_of(b), :] = error.astype(BF16)
        d_v[rows_of(b), :] = rms_back(new_state, -grad_scale * error).astype(BF16)
        return carry

    def backward(b, carry):
        u_v[rows_of(b), :] = (slope_v[rows_of(b), :] * dot_cols(d_v[rows_of(b), :], sd_v[...])).astype(BF16)
        return carry

    def gain_sum(b, carry):
        d_act = dot_cols(u_v[rows_of(b), :], su_v[...])
        small_v[0, 0:1, 0:s_width] += jnp.sum(d_act * rms_unit(state_of(b)), axis=0, keepdims=True)
        return carry

    lax.fori_loop(0, n_blk, forward, 0)
    g_v[:, 2 * f_width : 2 * f_width + t_width] = grad_scale * dot_rows(e_v[...], f_v[...])
    g_v[:, f_width : 2 * f_width] = dot_rows(d_v[...], u_v[...])
    run(group_a, 0)
    lax.fori_loop(0, n_blk, backward, 0)
    run(group_a, 1)
    g_v[:, 0:f_width] = dot_rows(act_v[...], u_v[...])
    run(group_b, 0)
    run(group_a, 2)
    lax.fori_loop(0, n_blk // 2, gain_sum, 0)
    run(group_b, 1)
    lax.fori_loop(n_blk // 2, n_blk, gain_sum, 0)
    small_v[0, 2:3, 0:PART] = jnp.broadcast_to(jnp.sum(small_v[0, 1:2, 0:s_width], axis=1, keepdims=True), (1, PART))
    small.send()
    for num in range(2, len(STAGES)):
        run(group_b, num)
        if num + 1 < len(STAGES):
            run(group_a, num + 1)
        if small.level <= len(STRIDES):
            small.add()
            if small.level <= len(STRIDES):
                small.send()
            else:
                small_out[...] = small_v[small.level]
    outs = [pltpu.make_async_copy(g_v.at[:, pl.ds(col, out.shape[1])], out, o_sem.at[i]) for i, (col, out) in enumerate([(0, up_out), (f_width, down_out), (2 * f_width, proj_out)])]
    for out in outs:
        out.start()
    for out in outs:
        out.wait()
    for copy in started:
        if copy is not None:
            copy.wait_send()


def sum_bufs(parts, n_cols):
    wide, vmem = n_cols // RING, pltpu.VMEM
    half, quarter = SIDE // 2, SIDE // RING
    shapes = [(SIDE, n_cols), (2, half, wide), (2, half, wide), (2, SIDE, wide), (SIDE, wide), (len(OTHERS), quarter, wide), (RING, quarter, wide)]
    return [vmem((parts,) + shape, F32) for shape in shapes]


def student_sums(feat, stud, stud_r, s_gain, s_up, s_down, s_proj, grad_scale):
    n_tok, width = feat.shape
    n_blk = n_tok // ROWS
    seqs, half_len, s_width = stud_r.shape
    f_width = s_up.shape[2]
    n_cols = 2 * f_width + width
    parts = s_width // PART
    dma = pltpu.SemaphoreType.DMA
    vmem = pltpu.VMEM
    v_act = vmem((n_tok, s_width), BF16)
    small = (8, s_width)
    n_copies = 200
    return pl.pallas_call(
        functools.partial(student_kernel, n_blk, grad_scale),
        out_shape=tuple(jax.ShapeDtypeStruct(shape, F32) for shape in ((s_width, f_width), (s_width, f_width), (s_width, width), small)),
        in_specs=any_specs(3) + [VM] + any_specs(3),
        out_specs=any_specs(3) + [VM],
        scratch_shapes=[
            vmem((n_tok, width), BF16), vmem((n_tok // half_len, half_len, s_width), BF16), vmem((s_width, f_width), BF16), vmem((f_width, s_width), BF16), vmem((width, s_width), BF16),
            vmem((n_tok, f_width), BF16), vmem((n_tok, f_width), F32), v_act, v_act, v_act, vmem((s_width, n_cols), F32), vmem((5,) + small, F32), vmem((4, 4) + small, F32)]
        + sum_bufs(parts, f_width + width) + sum_bufs(parts, f_width)
        + [dma((n_blk,)), dma((5,)), dma((3,)), dma((n_copies,)), dma((n_copies,)), pltpu.SemaphoreType.REGULAR((2, parts))],
        compiler_params=pltpu.CompilerParams(collective_id=2, has_side_effects=True, vmem_limit_bytes=VMEM_MAX),
        cost_estimate=pl.CostEstimate(flops=2**34, bytes_accessed=2**24, transcendentals=0),
        name="student_sums",
    )(feat, stud, stud_r, s_gain, s_up, s_down, s_proj)


def solution(mesh):
    dev_count = mesh.shape["data"] * mesh.shape["model"]

    def body(teacher_in, student_in, teacher_gain, teacher_up, teacher_down, student_gain, student_up, student_down, student_proj):
        seq_rows, seq_len, s_width = student_in.shape
        total = seq_rows * dev_count * seq_len * s_width
        grad_scale = 2.0 / total
        t_width = teacher_in.shape[2]
        feat, stud_r = teacher(teacher_in.reshape(-1, t_width), teacher_gain, teacher_up, teacher_down, student_in)
        grad_up, grad_down, grad_proj, small = student_sums(feat, student_in, stud_r, student_gain, student_up, student_down, student_proj, grad_scale)
        return (small[2, 0] / total, grad_up[None], grad_down.T[None], small[0:1, 0:s_width], grad_proj.T[None])

    return jax.shard_map(
        body,
        mesh=mesh,
        in_specs=(
            P("data", "model", None),
            P(("data", "model"), None, None),
            P(),
            P(None, None, "model"),
            P(None, "model", None),
            P(),
            P(),
            P(),
            P(),
        ),
        out_specs=(P(), P(), P(), P(), P()),
        check_vma=False,
    )
```

```python
import functools

import jax
import jax.numpy as jnp
from jax import lax
from jax.experimental import pallas as pl
from jax.experimental.pallas import tpu as pltpu
from jax.sharding import PartitionSpec as P

EPS = 1e-6
F32 = jnp.float32
BF16 = jnp.bfloat16
MESH = pl.DeviceIdType.MESH
ROWS = 512
VMEM_MAX = 62 * 2**20
GELU_A = 0.7978845608028654
GELU_B = 0.044715


def rms_unit(values):
    return values * lax.rsqrt(jnp.mean(values * values, axis=-1, keepdims=True) + EPS)


def rms_back(values, grad_out):
    inv_rms = lax.rsqrt(jnp.mean(values * values, axis=-1, keepdims=True) + EPS)
    unit = values * inv_rms
    return inv_rms * (grad_out - unit * jnp.mean(grad_out * unit, axis=-1, keepdims=True))


def gelu(pre):
    half = 0.5 * pre
    return half + half * jnp.tanh(pre * (GELU_A + (GELU_A * GELU_B) * (pre * pre)))


def rows_of(blk):
    return pl.ds(pl.multiple_of(blk * ROWS, ROWS), ROWS)


def partner():
    return {"model": 1 - lax.axis_index("model")}


def greet_partner():
    barrier = pltpu.get_barrier_semaphore()
    pl.semaphore_signal(barrier, inc=1, device_id=partner(), device_id_type=MESH)
    pl.semaphore_wait(barrier, 1)


def teacher_kernel(n_blk, h_in, gain, up, down, stud, f_out, stud_r, h_v, a_v, next_v, acc_v, p_v, up_v, down_v, h_sem, w_sem, o_sem, send_sem, recv_sem):
    half = up_v.shape[2] // 2
    n_tok = h_v.shape[0]

    def blk(b):
        return pl.ds(pl.multiple_of(b * ROWS, ROWS), ROWS)

    h_loads = [pltpu.make_async_copy(h_in.at[blk(b)], h_v.at[blk(b)], h_sem.at[b]) for b in range(n_blk)]
    w_loads = [
        [
            pltpu.make_async_copy(up.at[layer, :, pl.ds(part * half, half)], up_v.at[2 * layer, :, pl.ds(part * half, half)], w_sem.at[layer, part])
            for part in range(2)
        ]
        + [pltpu.make_async_copy(down.at[layer], down_v.at[2 * layer], w_sem.at[layer, 2])]
        for layer in range(2)
    ]
    for load in h_loads + w_loads[0]:
        load.start()
    greet_partner()
    swaps = []
    for layer in range(2):
        group = []
        for idx, (src, dst) in enumerate([(up, up_v), (down, down_v)]):
            step = src.shape[1] // 4
            for piece in range(4):
                rows = pl.ds(piece * step, step)
                sems = (layer, idx, piece)
                group.append(pltpu.make_async_remote_copy(
                    src_ref=src.at[layer, rows], dst_ref=dst.at[2 * layer + 1, rows],
                    send_sem=send_sem.at[sems], recv_sem=recv_sem.at[sems], device_id=partner(), device_id_type=MESH))
        swaps.append(group)
    for copy in swaps[0]:
        copy.start()
    for load in w_loads[1]:
        load.start()
    half_len = stud.shape[1] // 2
    give = pl.ds(pl.multiple_of((1 - lax.axis_index("model")) * half_len, half_len), half_len)
    last = (2, 0, 0)
    swaps[1].append(pltpu.make_async_remote_copy(src_ref=stud.at[:, give], dst_ref=stud_r, send_sem=send_sem.at[last], recv_sem=recv_sem.at[last], device_id=partner(), device_id_type=MESH))
    for copy in swaps[1]:
        copy.start()

    def normed(b, layer):
        return (rms_unit(h_v[blk(b), :].astype(F32)) * gain[pl.ds(layer, 1), :]).astype(BF16)

    def norm(b, layer):
        a_v[blk(b), :] = normed(b, layer)

    def up_part(unit, part):
        cols = pl.ds(part * half, half)
        p_v[part] = jnp.dot(a_v[blk(unit % n_blk), :], up_v[unit // n_blk, :, cols], preferred_element_type=F32)

    def down_part(unit, part):
        acc_v[blk(unit % n_blk), :] += jnp.dot(gelu(p_v[part]).astype(BF16), down_v[unit // n_blk, pl.ds(part * half, half), :], preferred_element_type=F32)

    def finish(b, layer):
        h_v[blk(b), :] = (h_v[blk(b), :].astype(F32) + acc_v[blk(b), :].astype(BF16).astype(F32)).astype(BF16)
        acc_v[blk(b), :] = jnp.zeros((ROWS, acc_v.shape[1]), F32)
        next_v[...] = normed(b, jnp.minimum(layer + 1, 1))

    def out(b):
        return pltpu.make_async_copy(h_v.at[blk(b)], f_out.at[blk(b)], o_sem.at[b])

    def clear(i, carry):
        acc_v[pl.ds(pl.multiple_of(i * 64, 64), 64), :] = jnp.zeros((64, acc_v.shape[1]), F32)
        return carry

    lax.fori_loop(0, n_tok // 64, clear, 0)
    h_loads[0].wait()
    norm(0, 0)
    w_loads[0][0].wait()
    up_part(0, 0)
    for load in h_loads[1:]:
        load.wait()

    def norm_step(b, carry):
        norm(b, 0)
        return carry

    lax.fori_loop(1, n_blk, norm_step, 0)
    for load in w_loads[0][1:]:
        load.wait()
    end = 4 * n_blk

    def arrive(unit, at, copies, remote):
        @pl.when(unit == at)
        def _():
            for copy in copies:
                if remote:
                    copy.wait_recv()
                else:
                    copy.wait()

    def layer_step(layer, carry):
        def plain(unit, inner):
            arrive(unit, n_blk - 1, swaps[0], True)
            arrive(unit, 3 * n_blk - 1, swaps[1], True)
            up_part(unit, 1)
            down_part(unit, 0)
            up_part(unit + 1, 0)
            down_part(unit, 1)
            return inner

        def closing(unit, inner):
            arrive(unit, 2 * n_blk - 1, w_loads[1], False)
            done = unit - (n_blk + 1) - 2 * n_blk * layer
            finish(done, layer)
            up_part(unit, 1)
            down_part(unit, 0)
            up_part(jnp.minimum(unit + 1, end - 1), 0)
            down_part(unit, 1)
            a_v[blk(done), :] = next_v[...]

            @pl.when(layer == 1)
            def _():
                out(done).start()

            return inner

        lax.fori_loop((2 * n_blk + 1) * layer, (n_blk + 1) + 2 * n_blk * layer, plain, 0)
        lax.fori_loop((n_blk + 1) + 2 * n_blk * layer, (2 * n_blk + 1) + (2 * n_blk - 1) * layer, closing, 0)
        return carry

    lax.fori_loop(0, 2, layer_step, 0)
    b_last = n_blk - 1
    h_v[blk(b_last), :] = (h_v[blk(b_last), :].astype(F32) + acc_v[blk(b_last), :].astype(BF16).astype(F32)).astype(BF16)
    out(b_last).start()
    for b in range(n_blk):
        out(b).wait()
    for group in swaps:
        for copy in group:
            copy.wait_send()


def any_specs(count):
    return [pl.BlockSpec(memory_space=pl.ANY)] * count


VM = pl.BlockSpec(memory_space=pltpu.VMEM)


def teacher(tokens, gain, up, down, stud):
    n_tok, width = tokens.shape
    cols = up.shape[2]
    n_blk = n_tok // ROWS
    seqs, length, s_width = stud.shape
    dma, vmem = pltpu.SemaphoreType.DMA, pltpu.VMEM
    v_tok = vmem((n_tok, width), BF16)
    return pl.pallas_call(
        functools.partial(teacher_kernel, n_blk),
        out_shape=(jax.ShapeDtypeStruct((n_tok, width), BF16), jax.ShapeDtypeStruct((seqs, length // 2, s_width), BF16)),
        in_specs=[pl.BlockSpec(memory_space=pl.ANY), VM] + any_specs(3),
        out_specs=any_specs(2),
        scratch_shapes=[v_tok, v_tok, vmem((ROWS, width), BF16), vmem((n_tok, width), F32), vmem((2, ROWS, cols // 2), F32), vmem((4, width, cols), BF16), vmem((4, cols, width), BF16),
                        dma((n_blk,)), dma((2, 3)), dma((n_blk,)), dma((3, 2, 4)), dma((3, 2, 4))],
        compiler_params=pltpu.CompilerParams(collective_id=0, has_side_effects=True, vmem_limit_bytes=VMEM_MAX),
        cost_estimate=pl.CostEstimate(flops=16 * n_tok * width * cols, bytes_accessed=2**25, transcendentals=0),
        name="teacher",
    )(tokens, gain, up, down, stud)


PART = 128
SIDE = PART // 2
RING = 4
STRIDES = (1, RING, RING * RING)
OTHERS = (2, 1, 3)


def gelu_pair(pre):
    sq = pre * pre
    tanh = jnp.tanh(pre * (GELU_A + (GELU_A * GELU_B) * sq))
    cdf = 0.5 + 0.5 * tanh
    slope = cdf + (0.5 * pre) * ((1.0 - tanh * tanh) * (GELU_A + (3.0 * GELU_A * GELU_B) * sq))
    return pre * cdf, slope


def dot_rows(lhs, rhs):
    return lax.dot_general(lhs, rhs, (((0,), (0,)), ((), ())), preferred_element_type=F32)


def dot_cols(lhs, rhs):
    return lax.dot_general(lhs, rhs, (((1,), (1,)), ((), ())), preferred_element_type=F32)


def axis_coord(stride):
    return (lax.axis_index("data") // stride) % RING


def axis_peer(stride, offset):
    coord = axis_coord(stride)
    return {"data": lax.axis_index("data") + (((coord + offset) % RING) - coord) * stride}


def span(index, size):
    return pl.ds(pl.multiple_of(index * size, size), size)


class PartSum:
    def __init__(self, ops, credit, g_v, bufs, part, first_col, n_cols):
        self.sender, self.credit, self.g_v, self.part = ops, credit, g_v, part
        self.core_v, self.fwd_v, self.fsum_v, self.near_v, self.p2_v, self.r2_v, self.slots_v = [buf.at[part] for buf in bufs]
        self.wide = n_cols // RING
        self.first_col, self.n_cols = first_col, n_cols
        self.axes = [STRIDES[(part + i) % len(STRIDES)] for i in range(len(STRIDES))]
        self.coords = [axis_coord(stride) for stride in self.axes]
        self.row0 = part * PART + lax.axis_index("model") * SIDE
        self.up, self.down = axis_peer(self.axes[0], 1), axis_peer(self.axes[0], RING - 1)
        self.cols = pl.ds(first_col, n_cols)

    def rows(self, offset, size):
        return pl.ds(pl.multiple_of(self.row0 + offset, size), size)

    def lanes(self, shift):
        return span((self.coords[0] + shift) % RING, self.wide)

    def out(self, offset, size, shift):
        lanes = pl.ds(pl.multiple_of(self.first_col + ((self.coords[0] + shift) % RING) * self.wide, 128), self.wide)
        return self.g_v.at[self.rows(offset, size), lanes]

    def core_send(self):
        away = pl.ds(pl.multiple_of(self.part * PART + (1 - lax.axis_index("model")) * SIDE, SIDE), SIDE)
        self.core = self.sender(self.g_v.at[away, self.cols], self.core_v, partner(), True)

    def ring_start(self):
        self.core.wait()
        pl.semaphore_signal(self.credit, inc=1, device_id=partner(), device_id_type=MESH)
        self.core_v[...] = self.core_v[...] + self.g_v[self.rows(0, SIDE), self.cols]
        half = SIDE // 2
        lo, hi = pl.ds(0, half), pl.ds(half, half)
        self.fwd = [self.sender(self.core_v.at[lo, self.lanes(2)], self.fwd_v.at[0], self.up), self.sender(self.core_v.at[hi, self.lanes(2)], self.fwd_v.at[1], self.down)]
        self.near = [self.sender(self.core_v.at[hi, self.lanes(1)], self.near_v.at[0, hi], self.up), self.sender(self.core_v.at[lo, self.lanes(3)], self.near_v.at[1, lo], self.down)]

    def ring_forward(self):
        half = SIDE // 2
        for which, shift, dev in ((0, 1, self.up), (1, 3, self.down)):
            rows = pl.ds(which * half, half)
            self.fwd[which].wait_recv()
            self.fsum_v[which] = self.fwd_v[which] + self.core_v[rows, self.lanes(shift)]
            self.near.append(self.sender(self.fsum_v.at[which], self.near_v.at[which, rows], dev))

    def second_start(self):
        for copy in self.near:
            copy.wait_recv()
        self.p2_v[...] = self.core_v[:, self.lanes(0)] + (self.near_v[0] + self.near_v[1])
        size = SIDE // RING
        self.r2 = [self.sender(self.p2_v.at[span((self.coords[1] + off) % RING, size)], self.r2_v.at[off - 1], axis_peer(self.axes[1], off)) for off in OTHERS]

    def third_start(self):
        for copy in self.r2:
            copy.wait_recv()
        slot = self.slots_v.at[self.coords[2]]
        slot[...] = (self.p2_v[span(self.coords[1], SIDE // RING), :] + self.r2_v[1]) + (self.r2_v[0] + self.r2_v[2])
        self.r3 = [self.sender(slot, slot, axis_peer(self.axes[2], off)) for off in OTHERS]

    def back_second(self):
        for copy in self.r3:
            copy.wait_recv()
        size = SIDE // RING
        block = self.out(self.coords[1] * size, size, 0)
        block[...] = (self.slots_v[0] + self.slots_v[1]) + (self.slots_v[2] + self.slots_v[3])
        self.b2 = [self.sender(block, block, axis_peer(self.axes[1], off)) for off in OTHERS]

    def back_first(self):
        for copy in self.b2:
            copy.wait_recv()
        half = SIDE // 2
        lo, hi = self.out(0, half, 0), self.out(half, half, 0)
        self.early = [self.sender(lo, lo, self.up), self.sender(hi, hi, self.down)]
        self.late = [self.sender(hi, hi, self.up), self.sender(lo, lo, self.down)]
        self.cross = []
        pl.semaphore_wait(self.credit, 1)
        self.give(0)

    def give(self, shift):
        block = self.out(0, SIDE, shift)
        self.cross.append(self.sender(block, block, partner()))

    def back_forward(self):
        half = SIDE // 2
        self.far = []
        for which, shift, dev in ((0, 3, self.up), (1, 1, self.down)):
            self.early[which].wait_recv()
            block = self.out(which * half, half, shift)
            self.far.append(self.sender(block, block, dev))

    def back_core(self):
        for which, shift in ((0, 3), (1, 1)):
            self.late[which].wait_recv()
            self.give(shift)

    def back_last(self):
        for copy in self.far:
            copy.wait_recv()
        self.give(2)

    def finish(self):
        for copy in self.cross:
            copy.wait_recv()


STAGES = ("core_send", "ring_start", "ring_forward", "second_start", "third_start", "back_second", "back_first", "back_forward", "back_core", "back_last", "finish")


class SmallSum:
    def __init__(self, sender, small_v, slots_v):
        self.sender, self.small_v, self.slots_v, self.level = sender, small_v, slots_v, 0

    def send(self):
        level = self.level
        coord = lax.axis_index("model") if level == 0 else axis_coord(STRIDES[level - 1])
        slots = self.slots_v.at[level]
        slots[coord] = self.small_v[level]
        peers = [partner()] if level == 0 else [axis_peer(STRIDES[level - 1], off) for off in OTHERS]
        self.copies = [self.sender(self.small_v.at[level], slots.at[coord], dev) for dev in peers]

    def add(self):
        for copy in self.copies:
            copy.wait_recv()
        slots = self.slots_v.at[self.level]
        total = slots[0] + slots[1]
        if self.level > 0:
            total = total + (slots[2] + slots[3])
        self.level += 1
        self.small_v[self.level] = total


def student_kernel(n_blk, grad_scale, f_in, stud, stud_r, s_gain, s_up, s_down, s_proj, up_out, down_out, proj_out, small_out, f_v, s_v, su_v, sd_v, sp_v, u_v, slope_v, act_v, d_v, e_v, g_v, small_v, slots_v, *rest):
    bufs_a, bufs_b = rest[:7], rest[7:14]
    f_sem, s_sem, o_sem, send_sem, recv_sem, credit = rest[14:]
    core = lax.axis_index("model")
    seqs, half_len, s_width = stud_r.shape
    f_width = s_up.shape[2]
    t_width = s_proj.shape[1]
    keep = span(core, half_len)
    f_loads = [pltpu.make_async_copy(f_in.at[rows_of(b)], f_v.at[rows_of(b)], f_sem.at[b]) for b in range(n_blk)]
    pairs = [(stud.at[:, keep], s_v.at[pl.ds(core * seqs, seqs)]), (stud_r, s_v.at[pl.ds((1 - core) * seqs, seqs)]), (s_up.at[0], su_v), (s_proj.at[0], sp_v), (s_down.at[0], sd_v)]
    s_loads = [pltpu.make_async_copy(src, dst, s_sem.at[i]) for i, (src, dst) in enumerate(pairs)]
    for load in s_loads + f_loads:
        load.start()
    barrier = pltpu.get_barrier_semaphore()
    peers = [partner()] + [axis_peer(stride, off) for stride in STRIDES for off in OTHERS]
    for peer in peers:
        pl.semaphore_signal(barrier, inc=1, device_id=peer, device_id_type=MESH)
    pl.semaphore_wait(barrier, len(peers))
    started = []

    def sender(src, dst, dev, waited=False):
        slot = len(started)
        copy = pltpu.make_async_remote_copy(src_ref=src, dst_ref=dst, send_sem=send_sem.at[slot], recv_sem=recv_sem.at[slot], device_id=dev, device_id_type=MESH)
        copy.start()
        started.append(None if waited else copy)
        return copy

    parts = range(s_width // PART)
    group_a = [PartSum(sender, credit.at[0, k], g_v, bufs_a, k, f_width, f_width + t_width) for k in parts]
    group_b = [PartSum(sender, credit.at[1, k], g_v, bufs_b, k, 0, f_width) for k in parts]
    small = SmallSum(sender, small_v, slots_v)

    def run(group, num):
        for part in group:
            getattr(part, STAGES[num])()

    small_v[0] = jnp.zeros(small_v.shape[1:], F32)
    for load in s_loads:
        load.wait()

    def state_of(b):
        n_seq = ROWS // half_len
        return s_v[pl.ds(b * n_seq, n_seq)].reshape(ROWS, s_width).astype(F32)

    def forward(b, carry):
        pltpu.make_async_copy(f_in.at[rows_of(b)], f_v.at[rows_of(b)], f_sem.at[b]).wait()
        state = state_of(b)
        target = jnp.dot(f_v[rows_of(b), :], sp_v[...], preferred_element_type=F32).astype(BF16)
        act = (rms_unit(state) * s_gain[...]).astype(BF16)
        act_v[rows_of(b), :] = act
        up_act, slope = gelu_pair(jnp.dot(act, su_v[...], preferred_element_type=F32))
        up_act = up_act.astype(BF16)
        slope_v[rows_of(b), :] = slope
        u_v[rows_of(b), :] = up_act
        new_state = (state + jnp.dot(up_act, sd_v[...], preferred_element_type=F32)).astype(BF16).astype(F32)
        error = target.astype(F32) - rms_unit(new_state)
        small_v[0, 1:2, 0:s_width] += jnp.sum(error * error, axis=0, keepdims=True)
        e_v[rows_of(b), :] = error.astype(BF16)
        d_v[rows_of(b), :] = rms_back(new_state, -grad_scale * error).astype(BF16)
        return carry

    def backward(b, carry):
        u_v[rows_of(b), :] = (slope_v[rows_of(b), :] * dot_cols(d_v[rows_of(b), :], sd_v[...])).astype(BF16)
        return carry

    def gain_sum(b, carry):
        d_act = dot_cols(u_v[rows_of(b), :], su_v[...])
        small_v[0, 0:1, 0:s_width] += jnp.sum(d_act * rms_unit(state_of(b)), axis=0, keepdims=True)
        return carry

    lax.fori_loop(0, n_blk, forward, 0)
    g_v[:, 2 * f_width : 2 * f_width + t_width] = grad_scale * dot_rows(e_v[...], f_v[...])
    g_v[:, f_width : 2 * f_width] = dot_rows(d_v[...], u_v[...])
    run(group_a, 0)
    lax.fori_loop(0, n_blk, backward, 0)
    run(group_a, 1)
    g_v[:, 0:f_width] = dot_rows(act_v[...], u_v[...])
    run(group_b, 0)
    run(group_a, 2)
    lax.fori_loop(0, n_blk // 2, gain_sum, 0)
    run(group_b, 1)
    lax.fori_loop(n_blk // 2, n_blk, gain_sum, 0)
    small_v[0, 2:3, 0:PART] = jnp.broadcast_to(jnp.sum(small_v[0, 1:2, 0:s_width], axis=1, keepdims=True), (1, PART))
    small.send()
    for num in range(2, len(STAGES)):
        run(group_b, num)
        if num + 1 < len(STAGES):
            run(group_a, num + 1)
        if small.level <= len(STRIDES):
            small.add()
            if small.level <= len(STRIDES):
                small.send()
            else:
                small_out[...] = small_v[small.level]
    outs = [pltpu.make_async_copy(g_v.at[:, pl.ds(col, out.shape[1])], out, o_sem.at[i]) for i, (col, out) in enumerate([(0, up_out), (f_width, down_out), (2 * f_width, proj_out)])]
    for out in outs:
        out.start()
    for out in outs:
        out.wait()
    for copy in started:
        if copy is not None:
            copy.wait_send()


def sum_bufs(parts, n_cols):
    wide, vmem = n_cols // RING, pltpu.VMEM
    half, quarter = SIDE // 2, SIDE // RING
    shapes = [(SIDE, n_cols), (2, half, wide), (2, half, wide), (2, SIDE, wide), (SIDE, wide), (len(OTHERS), quarter, wide), (RING, quarter, wide)]
    return [vmem((parts,) + shape, F32) for shape in shapes]


def student_sums(feat, stud, stud_r, s_gain, s_up, s_down, s_proj, grad_scale):
    n_tok, width = feat.shape
    n_blk = n_tok // ROWS
    seqs, half_len, s_width = stud_r.shape
    f_width = s_up.shape[2]
    n_cols = 2 * f_width + width
    parts = s_width // PART
    dma = pltpu.SemaphoreType.DMA
    vmem = pltpu.VMEM
    v_act = vmem((n_tok, s_width), BF16)
    small = (8, s_width)
    n_copies = 200
    return pl.pallas_call(
        functools.partial(student_kernel, n_blk, grad_scale),
        out_shape=tuple(jax.ShapeDtypeStruct(shape, F32) for shape in ((s_width, f_width), (s_width, f_width), (s_width, width), small)),
        in_specs=any_specs(3) + [VM] + any_specs(3),
        out_specs=any_specs(3) + [VM],
        scratch_shapes=[
            vmem((n_tok, width), BF16), vmem((n_tok // half_len, half_len, s_width), BF16), vmem((s_width, f_width), BF16), vmem((f_width, s_width), BF16), vmem((width, s_width), BF16),
            vmem((n_tok, f_width), BF16), vmem((n_tok, f_width), F32), v_act, v_act, v_act, vmem((s_width, n_cols), F32), vmem((5,) + small, F32), vmem((4, 4) + small, F32)]
        + sum_bufs(parts, f_width + width) + sum_bufs(parts, f_width)
        + [dma((n_blk,)), dma((5,)), dma((3,)), dma((n_copies,)), dma((n_copies,)), pltpu.SemaphoreType.REGULAR((2, parts))],
        compiler_params=pltpu.CompilerParams(collective_id=2, has_side_effects=True, vmem_limit_bytes=VMEM_MAX),
        cost_estimate=pl.CostEstimate(flops=2**34, bytes_accessed=2**24, transcendentals=0),
        name="student_sums",
    )(feat, stud, stud_r, s_gain, s_up, s_down, s_proj)


def unpack_kernel(inv_total, up_in, down_in, proj_in, small, up_out, down_out, proj_out, gain_out, loss_out):
    up_out[0] = up_in[...]
    down_out[0] = down_in[...].T
    proj_out[0] = proj_in[...].T
    gain_out[...] = small[0:1, :]
    loss_out[...] = small[2:3, 0:1] * inv_total


def unpack(grads_up, grads_down, grads_proj, small, total):
    rows, cols = grads_up.shape
    width = grads_proj.shape[1]
    steps = rows // PART

    def block(shape, index):
        return pl.BlockSpec(shape, index)

    return pl.pallas_call(
        functools.partial(unpack_kernel, 1.0 / total),
        grid=(steps,),
        out_shape=tuple(jax.ShapeDtypeStruct(shape, F32) for shape in ((1, rows, cols), (1, cols, rows), (1, width, rows), (1, rows), (1, 1))),
        in_specs=[block((PART, cols), lambda i: (i, 0)), block((PART, cols), lambda i: (i, 0)), block((PART, width), lambda i: (i, 0)), block(small.shape, lambda i: (0, 0))],
        out_specs=(block((1, PART, cols), lambda i: (0, i, 0)), block((1, cols, PART), lambda i: (0, 0, i)), block((1, width, PART), lambda i: (0, 0, i)), block((1, rows), lambda i: (0, 0)), block((1, 1), lambda i: (0, 0))),
        compiler_params=pltpu.CompilerParams(vmem_limit_bytes=VMEM_MAX),
        name="unpack",
    )(grads_up, grads_down, grads_proj, small)


def solution(mesh):
    dev_count = mesh.shape["data"] * mesh.shape["model"]

    def body(teacher_in, student_in, teacher_gain, teacher_up, teacher_down, student_gain, student_up, student_down, student_proj):
        seq_rows, seq_len, s_width = student_in.shape
        total = seq_rows * dev_count * seq_len * s_width
        grad_scale = 2.0 / total
        t_width = teacher_in.shape[2]
        feat, stud_r = teacher(teacher_in.reshape(-1, t_width), teacher_gain, teacher_up, teacher_down, student_in)
        grad_up, grad_down, grad_proj, small = student_sums(feat, student_in, stud_r, student_gain, student_up, student_down, student_proj, grad_scale)
        grad_up, grad_down, grad_proj, grad_gain, loss = unpack(grad_up, grad_down, grad_proj, small, total)
        return (loss[0, 0], grad_up, grad_down, grad_gain, grad_proj)

    return jax.shard_map(
        body,
        mesh=mesh,
        in_specs=(
            P("data", "model", None),
            P(("data", "model"), None, None),
            P(),
            P(None, None, "model"),
            P(None, "model", None),
            P(),
            P(),
            P(),
            P(),
        ),
        out_specs=(P(), P(), P(), P(), P()),
        check_vma=False,
    )
```

```python
import functools

import jax
import jax.numpy as jnp
from jax import lax
from jax.experimental import pallas as pl
from jax.experimental.pallas import tpu as pltpu
from jax.sharding import PartitionSpec as P

EPS = 1e-6
F32 = jnp.float32
BF16 = jnp.bfloat16
MESH = pl.DeviceIdType.MESH
ROWS = 512
VMEM_MAX = 62 * 2**20
GELU_A = 0.7978845608028654
GELU_B = 0.044715


def rms_unit(values):
    return values * lax.rsqrt(jnp.mean(values * values, axis=-1, keepdims=True) + EPS)


def rms_back(values, grad_out):
    inv_rms = lax.rsqrt(jnp.mean(values * values, axis=-1, keepdims=True) + EPS)
    unit = values * inv_rms
    return inv_rms * (grad_out - unit * jnp.mean(grad_out * unit, axis=-1, keepdims=True))


def gelu(pre):
    half = 0.5 * pre
    return half + half * jnp.tanh(pre * (GELU_A + (GELU_A * GELU_B) * (pre * pre)))


def rows_of(blk):
    return pl.ds(pl.multiple_of(blk * ROWS, ROWS), ROWS)


def partner():
    return {"model": 1 - lax.axis_index("model")}


def greet_partner():
    barrier = pltpu.get_barrier_semaphore()
    pl.semaphore_signal(barrier, inc=1, device_id=partner(), device_id_type=MESH)
    pl.semaphore_wait(barrier, 1)


def teacher_kernel(n_blk, h_in, gain, up, down, stud, f_out, stud_r, h_v, a_v, next_v, acc_v, p_v, up_v, down_v, h_sem, w_sem, o_sem, send_sem, recv_sem):
    half = up_v.shape[2] // 2
    n_tok = h_v.shape[0]

    def blk(b):
        return pl.ds(pl.multiple_of(b * ROWS, ROWS), ROWS)

    h_loads = [pltpu.make_async_copy(h_in.at[blk(b)], h_v.at[blk(b)], h_sem.at[b]) for b in range(n_blk)]
    w_loads = [
        [
            pltpu.make_async_copy(up.at[layer, :, pl.ds(part * half, half)], up_v.at[2 * layer, :, pl.ds(part * half, half)], w_sem.at[layer, part])
            for part in range(2)
        ]
        + [pltpu.make_async_copy(down.at[layer], down_v.at[2 * layer], w_sem.at[layer, 2])]
        for layer in range(2)
    ]
    for load in h_loads + w_loads[0]:
        load.start()
    greet_partner()
    swaps = []
    for layer in range(2):
        group = []
        for idx, (src, dst) in enumerate([(up, up_v), (down, down_v)]):
            step = src.shape[1] // 4
            for piece in range(4):
                rows = pl.ds(piece * step, step)
                sems = (layer, idx, piece)
                group.append(pltpu.make_async_remote_copy(
                    src_ref=src.at[layer, rows], dst_ref=dst.at[2 * layer + 1, rows],
                    send_sem=send_sem.at[sems], recv_sem=recv_sem.at[sems], device_id=partner(), device_id_type=MESH))
        swaps.append(group)
    for copy in swaps[0]:
        copy.start()
    for load in w_loads[1]:
        load.start()
    half_len = stud.shape[1] // 2
    give = pl.ds(pl.multiple_of((1 - lax.axis_index("model")) * half_len, half_len), half_len)
    last = (2, 0, 0)
    swaps[1].append(pltpu.make_async_remote_copy(src_ref=stud.at[:, give], dst_ref=stud_r, send_sem=send_sem.at[last], recv_sem=recv_sem.at[last], device_id=partner(), device_id_type=MESH))
    for copy in swaps[1]:
        copy.start()

    def normed(b, layer):
        return (rms_unit(h_v[blk(b), :].astype(F32)) * gain[pl.ds(layer, 1), :]).astype(BF16)

    def norm(b, layer):
        a_v[blk(b), :] = normed(b, layer)

    def up_part(unit, part):
        cols = pl.ds(part * half, half)
        p_v[part] = jnp.dot(a_v[blk(unit % n_blk), :], up_v[unit // n_blk, :, cols], preferred_element_type=F32)

    def down_part(unit, part):
        acc_v[blk(unit % n_blk), :] += jnp.dot(gelu(p_v[part]).astype(BF16), down_v[unit // n_blk, pl.ds(part * half, half), :], preferred_element_type=F32)

    def finish(b, layer):
        h_v[blk(b), :] = (h_v[blk(b), :].astype(F32) + acc_v[blk(b), :].astype(BF16).astype(F32)).astype(BF16)
        acc_v[blk(b), :] = jnp.zeros((ROWS, acc_v.shape[1]), F32)
        next_v[...] = normed(b, jnp.minimum(layer + 1, 1))

    def out(b):
        return pltpu.make_async_copy(h_v.at[blk(b)], f_out.at[blk(b)], o_sem.at[b])

    def clear(i, carry):
        acc_v[pl.ds(pl.multiple_of(i * 64, 64), 64), :] = jnp.zeros((64, acc_v.shape[1]), F32)
        return carry

    lax.fori_loop(0, n_tok // 64, clear, 0)
    h_loads[0].wait()
    norm(0, 0)
    w_loads[0][0].wait()
    up_part(0, 0)
    for load in h_loads[1:]:
        load.wait()

    def norm_step(b, carry):
        norm(b, 0)
        return carry

    lax.fori_loop(1, n_blk, norm_step, 0)
    for load in w_loads[0][1:]:
        load.wait()
    end = 4 * n_blk

    def arrive(unit, at, copies, remote):
        @pl.when(unit == at)
        def _():
            for copy in copies:
                if remote:
                    copy.wait_recv()
                else:
                    copy.wait()

    def layer_step(layer, carry):
        def plain(unit, inner):
            arrive(unit, n_blk - 1, swaps[0], True)
            arrive(unit, 3 * n_blk - 1, swaps[1], True)
            up_part(unit, 1)
            down_part(unit, 0)
            up_part(unit + 1, 0)
            down_part(unit, 1)
            return inner

        def closing(unit, inner):
            arrive(unit, 2 * n_blk - 1, w_loads[1], False)
            done = unit - (n_blk + 1) - 2 * n_blk * layer
            finish(done, layer)
            up_part(unit, 1)
            down_part(unit, 0)
            up_part(jnp.minimum(unit + 1, end - 1), 0)
            down_part(unit, 1)
            a_v[blk(done), :] = next_v[...]

            @pl.when(layer == 1)
            def _():
                out(done).start()

            return inner

        lax.fori_loop((2 * n_blk + 1) * layer, (n_blk + 1) + 2 * n_blk * layer, plain, 0)
        lax.fori_loop((n_blk + 1) + 2 * n_blk * layer, (2 * n_blk + 1) + (2 * n_blk - 1) * layer, closing, 0)
        return carry

    lax.fori_loop(0, 2, layer_step, 0)
    b_last = n_blk - 1
    h_v[blk(b_last), :] = (h_v[blk(b_last), :].astype(F32) + acc_v[blk(b_last), :].astype(BF16).astype(F32)).astype(BF16)
    out(b_last).start()
    for b in range(n_blk):
        out(b).wait()
    for group in swaps:
        for copy in group:
            copy.wait_send()


def any_specs(count):
    return [pl.BlockSpec(memory_space=pl.ANY)] * count


VM = pl.BlockSpec(memory_space=pltpu.VMEM)


def teacher(tokens, gain, up, down, stud):
    n_tok, width = tokens.shape
    cols = up.shape[2]
    n_blk = n_tok // ROWS
    seqs, length, s_width = stud.shape
    dma, vmem = pltpu.SemaphoreType.DMA, pltpu.VMEM
    v_tok = vmem((n_tok, width), BF16)
    return pl.pallas_call(
        functools.partial(teacher_kernel, n_blk),
        out_shape=(jax.ShapeDtypeStruct((n_tok, width), BF16), jax.ShapeDtypeStruct((seqs, length // 2, s_width), BF16)),
        in_specs=[pl.BlockSpec(memory_space=pl.ANY), VM] + any_specs(3),
        out_specs=any_specs(2),
        scratch_shapes=[v_tok, v_tok, vmem((ROWS, width), BF16), vmem((n_tok, width), F32), vmem((2, ROWS, cols // 2), F32), vmem((4, width, cols), BF16), vmem((4, cols, width), BF16),
                        dma((n_blk,)), dma((2, 3)), dma((n_blk,)), dma((3, 2, 4)), dma((3, 2, 4))],
        compiler_params=pltpu.CompilerParams(collective_id=0, has_side_effects=True, vmem_limit_bytes=VMEM_MAX),
        cost_estimate=pl.CostEstimate(flops=16 * n_tok * width * cols, bytes_accessed=2**25, transcendentals=0),
        name="teacher",
    )(tokens, gain, up, down, stud)


PART = 128
SIDE = PART // 2
RING = 4
STRIDES = (1, RING, RING * RING)
OTHERS = (2, 1, 3)


def gelu_pair(pre):
    sq = pre * pre
    tanh = jnp.tanh(pre * (GELU_A + (GELU_A * GELU_B) * sq))
    cdf = 0.5 + 0.5 * tanh
    slope = cdf + (0.5 * pre) * ((1.0 - tanh * tanh) * (GELU_A + (3.0 * GELU_A * GELU_B) * sq))
    return pre * cdf, slope


def dot_rows(lhs, rhs):
    return lax.dot_general(lhs, rhs, (((0,), (0,)), ((), ())), preferred_element_type=F32)


def dot_cols(lhs, rhs):
    return lax.dot_general(lhs, rhs, (((1,), (1,)), ((), ())), preferred_element_type=F32)


def axis_coord(stride):
    return (lax.axis_index("data") // stride) % RING


def axis_peer(stride, offset):
    coord = axis_coord(stride)
    return {"data": lax.axis_index("data") + (((coord + offset) % RING) - coord) * stride}


def span(index, size):
    return pl.ds(pl.multiple_of(index * size, size), size)


class PartSum:
    def __init__(self, ops, credit, g_v, bufs, part, first_col, n_cols):
        self.sender, self.credit, self.g_v, self.part = ops, credit, g_v, part
        self.core_v, self.fwd_v, self.fsum_v, self.near_v, self.p2_v, self.r2_v, self.slots_v = [buf.at[part] for buf in bufs]
        self.wide = n_cols // RING
        self.first_col, self.n_cols = first_col, n_cols
        self.axes = [STRIDES[(part + i) % len(STRIDES)] for i in range(len(STRIDES))]
        self.coords = [axis_coord(stride) for stride in self.axes]
        self.row0 = part * PART + lax.axis_index("model") * SIDE
        self.up, self.down = axis_peer(self.axes[0], 1), axis_peer(self.axes[0], RING - 1)
        self.cols = pl.ds(first_col, n_cols)

    def rows(self, offset, size):
        return pl.ds(pl.multiple_of(self.row0 + offset, size), size)

    def lanes(self, shift):
        return span((self.coords[0] + shift) % RING, self.wide)

    def out(self, offset, size, shift):
        lanes = pl.ds(pl.multiple_of(self.first_col + ((self.coords[0] + shift) % RING) * self.wide, 128), self.wide)
        return self.g_v.at[self.rows(offset, size), lanes]

    def core_send(self):
        away = pl.ds(pl.multiple_of(self.part * PART + (1 - lax.axis_index("model")) * SIDE, SIDE), SIDE)
        self.core = self.sender(self.g_v.at[away, self.cols], self.core_v, partner(), True)

    def ring_start(self):
        self.core.wait()
        pl.semaphore_signal(self.credit, inc=1, device_id=partner(), device_id_type=MESH)
        self.core_v[...] = self.core_v[...] + self.g_v[self.rows(0, SIDE), self.cols]
        half = SIDE // 2
        lo, hi = pl.ds(0, half), pl.ds(half, half)
        self.fwd = [self.sender(self.core_v.at[lo, self.lanes(2)], self.fwd_v.at[0], self.up), self.sender(self.core_v.at[hi, self.lanes(2)], self.fwd_v.at[1], self.down)]
        self.near = [self.sender(self.core_v.at[hi, self.lanes(1)], self.near_v.at[0, hi], self.up), self.sender(self.core_v.at[lo, self.lanes(3)], self.near_v.at[1, lo], self.down)]

    def ring_forward(self):
        half = SIDE // 2
        for which, shift, dev in ((0, 1, self.up), (1, 3, self.down)):
            rows = pl.ds(which * half, half)
            self.fwd[which].wait_recv()
            self.fsum_v[which] = self.fwd_v[which] + self.core_v[rows, self.lanes(shift)]
            self.near.append(self.sender(self.fsum_v.at[which], self.near_v.at[which, rows], dev))

    def second_start(self):
        for copy in self.near:
            copy.wait_recv()
        self.p2_v[...] = self.core_v[:, self.lanes(0)] + (self.near_v[0] + self.near_v[1])
        size = SIDE // RING
        self.r2 = [self.sender(self.p2_v.at[span((self.coords[1] + off) % RING, size)], self.r2_v.at[off - 1], axis_peer(self.axes[1], off)) for off in OTHERS]

    def third_start(self):
        for copy in self.r2:
            copy.wait_recv()
        slot = self.slots_v.at[self.coords[2]]
        slot[...] = (self.p2_v[span(self.coords[1], SIDE // RING), :] + self.r2_v[1]) + (self.r2_v[0] + self.r2_v[2])
        self.r3 = [self.sender(slot, slot, axis_peer(self.axes[2], off)) for off in OTHERS]

    def back_second(self):
        for copy in self.r3:
            copy.wait_recv()
        size = SIDE // RING
        block = self.out(self.coords[1] * size, size, 0)
        block[...] = (self.slots_v[0] + self.slots_v[1]) + (self.slots_v[2] + self.slots_v[3])
        self.b2 = [self.sender(block, block, axis_peer(self.axes[1], off)) for off in OTHERS]

    def back_first(self):
        for copy in self.b2:
            copy.wait_recv()
        half = SIDE // 2
        lo, hi = self.out(0, half, 0), self.out(half, half, 0)
        self.early = [self.sender(lo, lo, self.up), self.sender(hi, hi, self.down)]
        self.late = [self.sender(hi, hi, self.up), self.sender(lo, lo, self.down)]
        self.cross = []
        pl.semaphore_wait(self.credit, 1)
        self.give(0)

    def give(self, shift):
        block = self.out(0, SIDE, shift)
        self.cross.append(self.sender(block, block, partner()))

    def back_forward(self):
        half = SIDE // 2
        self.far = []
        for which, shift, dev in ((0, 3, self.up), (1, 1, self.down)):
            self.early[which].wait_recv()
            block = self.out(which * half, half, shift)
            self.far.append(self.sender(block, block, dev))

    def back_core(self):
        for which, shift in ((0, 3), (1, 1)):
            self.late[which].wait_recv()
            self.give(shift)

    def back_last(self):
        for copy in self.far:
            copy.wait_recv()
        self.give(2)

    def finish(self):
        for copy in self.cross:
            copy.wait_recv()


STAGES = ("core_send", "ring_start", "ring_forward", "second_start", "third_start", "back_second", "back_first", "back_forward", "back_core", "back_last", "finish")


class SmallSum:
    def __init__(self, sender, small_v, slots_v):
        self.sender, self.small_v, self.slots_v, self.level = sender, small_v, slots_v, 0

    def send(self):
        level = self.level
        coord = lax.axis_index("model") if level == 0 else axis_coord(STRIDES[level - 1])
        slots = self.slots_v.at[level]
        slots[coord] = self.small_v[level]
        peers = [partner()] if level == 0 else [axis_peer(STRIDES[level - 1], off) for off in OTHERS]
        self.copies = [self.sender(self.small_v.at[level], slots.at[coord], dev) for dev in peers]

    def add(self):
        for copy in self.copies:
            copy.wait_recv()
        slots = self.slots_v.at[self.level]
        total = slots[0] + slots[1]
        if self.level > 0:
            total = total + (slots[2] + slots[3])
        self.level += 1
        self.small_v[self.level] = total


def student_kernel(n_blk, grad_scale, f_in, stud, stud_r, s_gain, s_up, s_down, s_proj, up_out, down_out, proj_out, small_out, f_v, s_v, su_v, sd_v, sp_v, u_v, slope_v, act_v, d_v, e_v, g_v, small_v, slots_v, *rest):
    bufs_a, bufs_b = rest[:7], rest[7:14]
    f_sem, s_sem, o_sem, send_sem, recv_sem, credit = rest[14:]
    core = lax.axis_index("model")
    seqs, half_len, s_width = stud_r.shape
    f_width = s_up.shape[2]
    t_width = s_proj.shape[1]
    keep = span(core, half_len)
    f_loads = [pltpu.make_async_copy(f_in.at[rows_of(b)], f_v.at[rows_of(b)], f_sem.at[b]) for b in range(n_blk)]
    pairs = [(stud.at[:, keep], s_v.at[pl.ds(core * seqs, seqs)]), (stud_r, s_v.at[pl.ds((1 - core) * seqs, seqs)]), (s_up.at[0], su_v), (s_proj.at[0], sp_v), (s_down.at[0], sd_v)]
    s_loads = [pltpu.make_async_copy(src, dst, s_sem.at[i]) for i, (src, dst) in enumerate(pairs)]
    for load in s_loads + f_loads:
        load.start()
    barrier = pltpu.get_barrier_semaphore()
    peers = [partner()] + [axis_peer(stride, off) for stride in STRIDES for off in OTHERS]
    for peer in peers:
        pl.semaphore_signal(barrier, inc=1, device_id=peer, device_id_type=MESH)
    pl.semaphore_wait(barrier, len(peers))
    started = []

    def sender(src, dst, dev, waited=False):
        slot = len(started)
        copy = pltpu.make_async_remote_copy(src_ref=src, dst_ref=dst, send_sem=send_sem.at[slot], recv_sem=recv_sem.at[slot], device_id=dev, device_id_type=MESH)
        copy.start()
        started.append(None if waited else copy)
        return copy

    parts = range(s_width // PART)
    group_a = [PartSum(sender, credit.at[0, k], g_v, bufs_a, k, f_width, f_width + t_width) for k in parts]
    group_b = [PartSum(sender, credit.at[1, k], g_v, bufs_b, k, 0, f_width) for k in parts]
    small = SmallSum(sender, small_v, slots_v)

    def run(group, num):
        for part in group:
            getattr(part, STAGES[num])()

    small_v[0] = jnp.zeros(small_v.shape[1:], F32)
    for load in s_loads:
        load.wait()

    def state_of(b):
        n_seq = ROWS // half_len
        return s_v[pl.ds(b * n_seq, n_seq)].reshape(ROWS, s_width).astype(F32)

    def forward(b, carry):
        pltpu.make_async_copy(f_in.at[rows_of(b)], f_v.at[rows_of(b)], f_sem.at[b]).wait()
        state = state_of(b)
        target = jnp.dot(f_v[rows_of(b), :], sp_v[...], preferred_element_type=F32).astype(BF16)
        act = (rms_unit(state) * s_gain[...]).astype(BF16)
        act_v[rows_of(b), :] = act
        up_act, slope = gelu_pair(jnp.dot(act, su_v[...], preferred_element_type=F32))
        up_act = up_act.astype(BF16)
        slope_v[rows_of(b), :] = slope
        u_v[rows_of(b), :] = up_act
        new_state = (state + jnp.dot(up_act, sd_v[...], preferred_element_type=F32)).astype(BF16).astype(F32)
        error = target.astype(F32) - rms_unit(new_state)
        small_v[0, 1:2, 0:s_width] += jnp.sum(error * error, axis=0, keepdims=True)
        e_v[rows_of(b), :] = error.astype(BF16)
        d_v[rows_of(b), :] = rms_back(new_state, -grad_scale * error).astype(BF16)
        return carry

    def backward(b, carry):
        u_v[rows_of(b), :] = (slope_v[rows_of(b), :] * dot_cols(d_v[rows_of(b), :], sd_v[...])).astype(BF16)
        return carry

    def gain_sum(b, carry):
        d_act = dot_cols(u_v[rows_of(b), :], su_v[...])
        small_v[0, 0:1, 0:s_width] += jnp.sum(d_act * rms_unit(state_of(b)), axis=0, keepdims=True)
        return carry

    lax.fori_loop(0, n_blk, forward, 0, unroll=2)
    g_v[:, 2 * f_width : 2 * f_width + t_width] = grad_scale * dot_rows(e_v[...], f_v[...])
    g_v[:, f_width : 2 * f_width] = dot_rows(d_v[...], u_v[...])
    run(group_a, 0)
    lax.fori_loop(0, n_blk, backward, 0, unroll=2)
    run(group_a, 1)
    g_v[:, 0:f_width] = dot_rows(act_v[...], u_v[...])
    run(group_b, 0)
    run(group_a, 2)
    lax.fori_loop(0, n_blk // 2, gain_sum, 0)
    run(group_b, 1)
    lax.fori_loop(n_blk // 2, n_blk, gain_sum, 0)
    small_v[0, 2:3, 0:PART] = jnp.broadcast_to(jnp.sum(small_v[0, 1:2, 0:s_width], axis=1, keepdims=True), (1, PART))
    small.send()
    stores = [pltpu.make_async_copy(g_v.at[:, pl.ds(col, out.shape[1])], out, o_sem.at[i]) for i, (col, out) in enumerate([(0, up_out), (f_width, down_out), (2 * f_width, proj_out)])]
    final = len(STAGES) - 1
    for num in range(2, len(STAGES)):
        run(group_b, num)
        if num == final:
            stores[0].start()
        if num < final:
            run(group_a, num + 1)
            if num + 1 == final:
                stores[1].start()
                stores[2].start()
        if small.level <= len(STRIDES):
            small.add()
            if small.level <= len(STRIDES):
                small.send()
            else:
                small_out[...] = small_v[small.level]
    for store in stores:
        store.wait()
    for copy in started:
        if copy is not None:
            copy.wait_send()


def sum_bufs(parts, n_cols):
    wide, vmem = n_cols // RING, pltpu.VMEM
    half, quarter = SIDE // 2, SIDE // RING
    shapes = [(SIDE, n_cols), (2, half, wide), (2, half, wide), (2, SIDE, wide), (SIDE, wide), (len(OTHERS), quarter, wide), (RING, quarter, wide)]
    return [vmem((parts,) + shape, F32) for shape in shapes]


def student_sums(feat, stud, stud_r, s_gain, s_up, s_down, s_proj, grad_scale):
    n_tok, width = feat.shape
    n_blk = n_tok // ROWS
    seqs, half_len, s_width = stud_r.shape
    f_width = s_up.shape[2]
    n_cols = 2 * f_width + width
    parts = s_width // PART
    dma = pltpu.SemaphoreType.DMA
    vmem = pltpu.VMEM
    v_act = vmem((n_tok, s_width), BF16)
    small = (8, s_width)
    n_copies = 200
    return pl.pallas_call(
        functools.partial(student_kernel, n_blk, grad_scale),
        out_shape=tuple(jax.ShapeDtypeStruct(shape, F32) for shape in ((s_width, f_width), (s_width, f_width), (s_width, width), small)),
        in_specs=any_specs(3) + [VM] + any_specs(3),
        out_specs=any_specs(3) + [VM],
        scratch_shapes=[
            vmem((n_tok, width), BF16), vmem((n_tok // half_len, half_len, s_width), BF16), vmem((s_width, f_width), BF16), vmem((f_width, s_width), BF16), vmem((width, s_width), BF16),
            vmem((n_tok, f_width), BF16), vmem((n_tok, f_width), F32), v_act, v_act, v_act, vmem((s_width, n_cols), F32), vmem((5,) + small, F32), vmem((4, 4) + small, F32)]
        + sum_bufs(parts, f_width + width) + sum_bufs(parts, f_width)
        + [dma((n_blk,)), dma((5,)), dma((3,)), dma((n_copies,)), dma((n_copies,)), pltpu.SemaphoreType.REGULAR((2, parts))],
        compiler_params=pltpu.CompilerParams(collective_id=2, has_side_effects=True, vmem_limit_bytes=VMEM_MAX),
        cost_estimate=pl.CostEstimate(flops=2**34, bytes_accessed=2**24, transcendentals=0),
        name="student_sums",
    )(feat, stud, stud_r, s_gain, s_up, s_down, s_proj)


def unpack_kernel(inv_total, up_in, down_in, proj_in, small, up_out, down_out, proj_out, gain_out, loss_out):
    up_out[0] = up_in[...]
    down_out[0] = down_in[...].T
    proj_out[0] = proj_in[...].T
    gain_out[...] = small[0:1, :]
    loss_out[...] = small[2:3, 0:1] * inv_total


def unpack(grads_up, grads_down, grads_proj, small, total):
    rows, cols = grads_up.shape
    width = grads_proj.shape[1]
    steps = 2
    col, wid = cols // steps, width // steps

    def block(shape, index):
        return pl.BlockSpec(shape, index)

    return pl.pallas_call(
        functools.partial(unpack_kernel, 1.0 / total),
        grid=(steps,),
        out_shape=tuple(jax.ShapeDtypeStruct(shape, F32) for shape in ((1, rows, cols), (1, cols, rows), (1, width, rows), (1, rows), (1, 1))),
        in_specs=[block((rows, col), lambda i: (0, i)), block((rows, col), lambda i: (0, i)), block((rows, wid), lambda i: (0, i)), block(small.shape, lambda i: (0, 0))],
        out_specs=(block((1, rows, col), lambda i: (0, 0, i)), block((1, col, rows), lambda i: (0, i, 0)), block((1, wid, rows), lambda i: (0, i, 0)), block((1, rows), lambda i: (0, 0)), block((1, 1), lambda i: (0, 0))),
        compiler_params=pltpu.CompilerParams(vmem_limit_bytes=VMEM_MAX),
        name="unpack",
    )(grads_up, grads_down, grads_proj, small)


def solution(mesh):
    dev_count = mesh.shape["data"] * mesh.shape["model"]

    def body(teacher_in, student_in, teacher_gain, teacher_up, teacher_down, student_gain, student_up, student_down, student_proj):
        seq_rows, seq_len, s_width = student_in.shape
        total = seq_rows * dev_count * seq_len * s_width
        grad_scale = 2.0 / total
        t_width = teacher_in.shape[2]
        feat, stud_r = teacher(teacher_in.reshape(-1, t_width), teacher_gain, teacher_up, teacher_down, student_in)
        grad_up, grad_down, grad_proj, small = student_sums(feat, student_in, stud_r, student_gain, student_up, student_down, student_proj, grad_scale)
        grad_up, grad_down, grad_proj, grad_gain, loss = unpack(grad_up, grad_down, grad_proj, small, total)
        return (loss[0, 0], grad_up, grad_down, grad_gain, grad_proj)

    return jax.shard_map(
        body,
        mesh=mesh,
        in_specs=(
            P("data", "model", None),
            P(("data", "model"), None, None),
            P(),
            P(None, None, "model"),
            P(None, "model", None),
            P(),
            P(),
            P(),
            P(),
        ),
        out_specs=(P(), P(), P(), P(), P()),
        check_vma=False,
    )
```

```python
import functools

import jax
import jax.numpy as jnp
from jax import lax
from jax.experimental import pallas as pl
from jax.experimental.pallas import tpu as pltpu
from jax.sharding import PartitionSpec as P

EPS = 1e-6
F32 = jnp.float32
BF16 = jnp.bfloat16
MESH = pl.DeviceIdType.MESH
ROWS = 512
VMEM_MAX = 62 * 2**20
GELU_A = 0.7978845608028654
GELU_B = 0.044715


def rms_unit(values):
    return values * lax.rsqrt(jnp.mean(values * values, axis=-1, keepdims=True) + EPS)


def rms_back(values, grad_out):
    inv_rms = lax.rsqrt(jnp.mean(values * values, axis=-1, keepdims=True) + EPS)
    unit = values * inv_rms
    return inv_rms * (grad_out - unit * jnp.mean(grad_out * unit, axis=-1, keepdims=True))


def gelu(pre):
    half = 0.5 * pre
    return half + half * jnp.tanh(pre * (GELU_A + (GELU_A * GELU_B) * (pre * pre)))


def rows_of(blk):
    return pl.ds(pl.multiple_of(blk * ROWS, ROWS), ROWS)


def partner():
    return {"model": 1 - lax.axis_index("model")}


def greet_partner():
    barrier = pltpu.get_barrier_semaphore()
    pl.semaphore_signal(barrier, inc=1, device_id=partner(), device_id_type=MESH)
    pl.semaphore_wait(barrier, 1)


def teacher_kernel(n_blk, h_in, gain, up, down, stud, f_out, stud_r, h_v, a_v, next_v, acc_v, p_v, up_v, down_v, h_sem, w_sem, o_sem, send_sem, recv_sem):
    half = up_v.shape[2] // 2
    n_tok = h_v.shape[0]

    def blk(b):
        return pl.ds(pl.multiple_of(b * ROWS, ROWS), ROWS)

    h_loads = [pltpu.make_async_copy(h_in.at[blk(b)], h_v.at[blk(b)], h_sem.at[b]) for b in range(n_blk)]
    w_loads = [
        [
            pltpu.make_async_copy(up.at[layer, :, pl.ds(part * half, half)], up_v.at[2 * layer, :, pl.ds(part * half, half)], w_sem.at[layer, part])
            for part in range(2)
        ]
        + [pltpu.make_async_copy(down.at[layer], down_v.at[2 * layer], w_sem.at[layer, 2])]
        for layer in range(2)
    ]
    for load in h_loads + w_loads[0]:
        load.start()
    greet_partner()
    swaps = []
    for layer in range(2):
        group = []
        for idx, (src, dst) in enumerate([(up, up_v), (down, down_v)]):
            step = src.shape[1] // 4
            for piece in range(4):
                rows = pl.ds(piece * step, step)
                sems = (layer, idx, piece)
                group.append(pltpu.make_async_remote_copy(
                    src_ref=src.at[layer, rows], dst_ref=dst.at[2 * layer + 1, rows],
                    send_sem=send_sem.at[sems], recv_sem=recv_sem.at[sems], device_id=partner(), device_id_type=MESH))
        swaps.append(group)
    for copy in swaps[0]:
        copy.start()
    for load in w_loads[1]:
        load.start()
    half_len = stud.shape[1] // 2
    give = pl.ds(pl.multiple_of((1 - lax.axis_index("model")) * half_len, half_len), half_len)
    last = (2, 0, 0)
    swaps[1].append(pltpu.make_async_remote_copy(src_ref=stud.at[:, give], dst_ref=stud_r, send_sem=send_sem.at[last], recv_sem=recv_sem.at[last], device_id=partner(), device_id_type=MESH))
    for copy in swaps[1]:
        copy.start()

    def normed(b, layer):
        return (rms_unit(h_v[blk(b), :].astype(F32)) * gain[pl.ds(layer, 1), :]).astype(BF16)

    def norm(b, layer):
        a_v[blk(b), :] = normed(b, layer)

    def up_part(unit, part):
        cols = pl.ds(part * half, half)
        p_v[part] = jnp.dot(a_v[blk(unit % n_blk), :], up_v[unit // n_blk, :, cols], preferred_element_type=F32)

    def down_part(unit, part):
        acc_v[blk(unit % n_blk), :] += jnp.dot(gelu(p_v[part]).astype(BF16), down_v[unit // n_blk, pl.ds(part * half, half), :], preferred_element_type=F32)

    def finish(b, layer):
        h_v[blk(b), :] = (h_v[blk(b), :].astype(F32) + acc_v[blk(b), :].astype(BF16).astype(F32)).astype(BF16)
        acc_v[blk(b), :] = jnp.zeros((ROWS, acc_v.shape[1]), F32)
        next_v[...] = normed(b, jnp.minimum(layer + 1, 1))

    def out(b):
        return pltpu.make_async_copy(h_v.at[blk(b)], f_out.at[blk(b)], o_sem.at[b])

    def clear(i, carry):
        acc_v[pl.ds(pl.multiple_of(i * 64, 64), 64), :] = jnp.zeros((64, acc_v.shape[1]), F32)
        return carry

    lax.fori_loop(0, n_tok // 64, clear, 0)
    h_loads[0].wait()
    norm(0, 0)
    w_loads[0][0].wait()
    up_part(0, 0)
    for load in h_loads[1:]:
        load.wait()

    def norm_step(b, carry):
        norm(b, 0)
        return carry

    lax.fori_loop(1, n_blk, norm_step, 0)
    for load in w_loads[0][1:]:
        load.wait()
    end = 4 * n_blk

    def arrive(unit, at, copies, remote):
        @pl.when(unit == at)
        def _():
            for copy in copies:
                if remote:
                    copy.wait_recv()
                else:
                    copy.wait()

    def layer_step(layer, carry):
        def plain(unit, inner):
            arrive(unit, n_blk - 1, swaps[0], True)
            arrive(unit, 3 * n_blk - 1, swaps[1], True)
            up_part(unit, 1)
            down_part(unit, 0)
            up_part(unit + 1, 0)
            down_part(unit, 1)
            return inner

        def closing(unit, inner):
            arrive(unit, 2 * n_blk - 1, w_loads[1], False)
            done = unit - (n_blk + 1) - 2 * n_blk * layer
            finish(done, layer)
            up_part(unit, 1)
            down_part(unit, 0)
            up_part(unit + 1, 0)
            down_part(unit, 1)
            a_v[blk(done), :] = next_v[...]

            @pl.when(layer == 1)
            def _():
                out(done).start()

            return inner

        lax.fori_loop((2 * n_blk + 1) * layer, (n_blk + 1) + 2 * n_blk * layer, plain, 0)
        lax.fori_loop((n_blk + 1) + 2 * n_blk * layer, (2 * n_blk + 1) + 2 * (n_blk - 1) * layer, closing, 0)
        return carry

    lax.fori_loop(0, 2, layer_step, 0)

    def close(b):
        h_v[blk(b), :] = (h_v[blk(b), :].astype(F32) + acc_v[blk(b), :].astype(BF16).astype(F32)).astype(BF16)
        out(b).start()

    close(n_blk - 2)
    up_part(end - 1, 1)
    down_part(end - 1, 0)
    down_part(end - 1, 1)
    close(n_blk - 1)
    for b in range(n_blk):
        out(b).wait()
    for group in swaps:
        for copy in group:
            copy.wait_send()


def any_specs(count):
    return [pl.BlockSpec(memory_space=pl.ANY)] * count


VM = pl.BlockSpec(memory_space=pltpu.VMEM)


def teacher(tokens, gain, up, down, stud):
    n_tok, width = tokens.shape
    cols = up.shape[2]
    n_blk = n_tok // ROWS
    seqs, length, s_width = stud.shape
    dma, vmem = pltpu.SemaphoreType.DMA, pltpu.VMEM
    v_tok = vmem((n_tok, width), BF16)
    return pl.pallas_call(
        functools.partial(teacher_kernel, n_blk),
        out_shape=(jax.ShapeDtypeStruct((n_tok, width), BF16), jax.ShapeDtypeStruct((seqs, length // 2, s_width), BF16)),
        in_specs=[pl.BlockSpec(memory_space=pl.ANY), VM] + any_specs(3),
        out_specs=any_specs(2),
        scratch_shapes=[v_tok, v_tok, vmem((ROWS, width), BF16), vmem((n_tok, width), F32), vmem((2, ROWS, cols // 2), F32), vmem((4, width, cols), BF16), vmem((4, cols, width), BF16),
                        dma((n_blk,)), dma((2, 3)), dma((n_blk,)), dma((3, 2, 4)), dma((3, 2, 4))],
        compiler_params=pltpu.CompilerParams(collective_id=0, has_side_effects=True, vmem_limit_bytes=VMEM_MAX),
        cost_estimate=pl.CostEstimate(flops=16 * n_tok * width * cols, bytes_accessed=2**25, transcendentals=0),
        name="teacher",
    )(tokens, gain, up, down, stud)


PART = 128
SIDE = PART // 2
RING = 4
STRIDES = (1, RING, RING * RING)
OTHERS = (2, 1, 3)


def gelu_pair(pre):
    sq = pre * pre
    tanh = jnp.tanh(pre * (GELU_A + (GELU_A * GELU_B) * sq))
    cdf = 0.5 + 0.5 * tanh
    slope = cdf + (0.5 * pre) * ((1.0 - tanh * tanh) * (GELU_A + (3.0 * GELU_A * GELU_B) * sq))
    return pre * cdf, slope


def dot_rows(lhs, rhs):
    return lax.dot_general(lhs, rhs, (((0,), (0,)), ((), ())), preferred_element_type=F32)


def dot_cols(lhs, rhs):
    return lax.dot_general(lhs, rhs, (((1,), (1,)), ((), ())), preferred_element_type=F32)


def axis_coord(stride):
    return (lax.axis_index("data") // stride) % RING


def axis_peer(stride, offset):
    coord = axis_coord(stride)
    return {"data": lax.axis_index("data") + (((coord + offset) % RING) - coord) * stride}


def span(index, size):
    return pl.ds(pl.multiple_of(index * size, size), size)


class PartSum:
    def __init__(self, ops, credit, g_v, bufs, part, first_col, n_cols):
        self.sender, self.credit, self.g_v, self.part = ops, credit, g_v, part
        self.core_v, self.fwd_v, self.fsum_v, self.near_v, self.p2_v, self.r2_v, self.slots_v = [buf.at[part] for buf in bufs]
        self.wide = n_cols // RING
        self.first_col, self.n_cols = first_col, n_cols
        self.axes = [STRIDES[(part + i) % len(STRIDES)] for i in range(len(STRIDES))]
        self.coords = [axis_coord(stride) for stride in self.axes]
        self.row0 = part * PART + lax.axis_index("model") * SIDE
        self.up, self.down = axis_peer(self.axes[0], 1), axis_peer(self.axes[0], RING - 1)
        self.cols = pl.ds(first_col, n_cols)

    def rows(self, offset, size):
        return pl.ds(pl.multiple_of(self.row0 + offset, size), size)

    def lanes(self, shift):
        return span((self.coords[0] + shift) % RING, self.wide)

    def out(self, offset, size, shift):
        lanes = pl.ds(pl.multiple_of(self.first_col + ((self.coords[0] + shift) % RING) * self.wide, 128), self.wide)
        return self.g_v.at[self.rows(offset, size), lanes]

    def core_send(self):
        away = pl.ds(pl.multiple_of(self.part * PART + (1 - lax.axis_index("model")) * SIDE, SIDE), SIDE)
        self.core = self.sender(self.g_v.at[away, self.cols], self.core_v, partner(), True)

    def ring_start(self):
        self.core.wait()
        pl.semaphore_signal(self.credit, inc=1, device_id=partner(), device_id_type=MESH)
        self.core_v[...] = self.core_v[...] + self.g_v[self.rows(0, SIDE), self.cols]
        half = SIDE // 2
        lo, hi = pl.ds(0, half), pl.ds(half, half)
        self.fwd = [self.sender(self.core_v.at[lo, self.lanes(2)], self.fwd_v.at[0], self.up), self.sender(self.core_v.at[hi, self.lanes(2)], self.fwd_v.at[1], self.down)]
        self.near = [self.sender(self.core_v.at[hi, self.lanes(1)], self.near_v.at[0, hi], self.up), self.sender(self.core_v.at[lo, self.lanes(3)], self.near_v.at[1, lo], self.down)]

    def ring_forward(self):
        half = SIDE // 2
        for which, shift, dev in ((0, 1, self.up), (1, 3, self.down)):
            rows = pl.ds(which * half, half)
            self.fwd[which].wait_recv()
            self.fsum_v[which] = self.fwd_v[which] + self.core_v[rows, self.lanes(shift)]
            self.near.append(self.sender(self.fsum_v.at[which], self.near_v.at[which, rows], dev))

    def second_start(self):
        for copy in self.near:
            copy.wait_recv()
        self.p2_v[...] = self.core_v[:, self.lanes(0)] + (self.near_v[0] + self.near_v[1])
        size = SIDE // RING
        self.r2 = [self.sender(self.p2_v.at[span((self.coords[1] + off) % RING, size)], self.r2_v.at[off - 1], axis_peer(self.axes[1], off)) for off in OTHERS]

    def third_start(self):
        for copy in self.r2:
            copy.wait_recv()
        slot = self.slots_v.at[self.coords[2]]
        slot[...] = (self.p2_v[span(self.coords[1], SIDE // RING), :] + self.r2_v[1]) + (self.r2_v[0] + self.r2_v[2])
        self.r3 = [self.sender(slot, slot, axis_peer(self.axes[2], off)) for off in OTHERS]

    def back_second(self):
        for copy in self.r3:
            copy.wait_recv()
        size = SIDE // RING
        block = self.out(self.coords[1] * size, size, 0)
        block[...] = (self.slots_v[0] + self.slots_v[1]) + (self.slots_v[2] + self.slots_v[3])
        self.b2 = [self.sender(block, block, axis_peer(self.axes[1], off)) for off in OTHERS]

    def back_first(self):
        for copy in self.b2:
            copy.wait_recv()
        half = SIDE // 2
        lo, hi = self.out(0, half, 0), self.out(half, half, 0)
        self.early = [self.sender(lo, lo, self.up), self.sender(hi, hi, self.down)]
        self.late = [self.sender(hi, hi, self.up), self.sender(lo, lo, self.down)]
        self.cross = []
        pl.semaphore_wait(self.credit, 1)
        self.give(0)

    def give(self, shift):
        block = self.out(0, SIDE, shift)
        self.cross.append(self.sender(block, block, partner()))

    def back_forward(self):
        half = SIDE // 2
        self.far = []
        for which, shift, dev in ((0, 3, self.up), (1, 1, self.down)):
            self.early[which].wait_recv()
            block = self.out(which * half, half, shift)
            self.far.append(self.sender(block, block, dev))

    def back_core(self):
        for which, shift in ((0, 3), (1, 1)):
            self.late[which].wait_recv()
            self.give(shift)

    def back_last(self):
        for copy in self.far:
            copy.wait_recv()
        self.give(2)

    def finish(self):
        for copy in self.cross:
            copy.wait_recv()


STAGES = ("core_send", "ring_start", "ring_forward", "second_start", "third_start", "back_second", "back_first", "back_forward", "back_core", "back_last", "finish")


class SmallSum:
    def __init__(self, sender, small_v, slots_v):
        self.sender, self.small_v, self.slots_v, self.level = sender, small_v, slots_v, 0

    def send(self):
        level = self.level
        coord = lax.axis_index("model") if level == 0 else axis_coord(STRIDES[level - 1])
        slots = self.slots_v.at[level]
        slots[coord] = self.small_v[level]
        peers = [partner()] if level == 0 else [axis_peer(STRIDES[level - 1], off) for off in OTHERS]
        self.copies = [self.sender(self.small_v.at[level], slots.at[coord], dev) for dev in peers]

    def add(self):
        for copy in self.copies:
            copy.wait_recv()
        slots = self.slots_v.at[self.level]
        total = slots[0] + slots[1]
        if self.level > 0:
            total = total + (slots[2] + slots[3])
        self.level += 1
        self.small_v[self.level] = total


def student_kernel(n_blk, grad_scale, f_in, stud, stud_r, s_gain, s_up, s_down, s_proj, up_out, down_out, proj_out, small_out, f_v, s_v, su_v, sd_v, sp_v, u_v, slope_v, act_v, d_v, e_v, g_v, small_v, slots_v, *rest):
    bufs_a, bufs_b = rest[:7], rest[7:14]
    f_sem, s_sem, o_sem, send_sem, recv_sem, credit = rest[14:]
    core = lax.axis_index("model")
    seqs, half_len, s_width = stud_r.shape
    f_width = s_up.shape[2]
    t_width = s_proj.shape[1]
    keep = span(core, half_len)
    f_loads = [pltpu.make_async_copy(f_in.at[rows_of(b)], f_v.at[rows_of(b)], f_sem.at[b]) for b in range(n_blk)]
    pairs = [(stud.at[:, keep], s_v.at[pl.ds(core * seqs, seqs)]), (stud_r, s_v.at[pl.ds((1 - core) * seqs, seqs)]), (s_up.at[0], su_v), (s_proj.at[0], sp_v), (s_down.at[0], sd_v)]
    s_loads = [pltpu.make_async_copy(src, dst, s_sem.at[i]) for i, (src, dst) in enumerate(pairs)]
    for load in s_loads + f_loads:
        load.start()
    barrier = pltpu.get_barrier_semaphore()
    peers = [partner()] + [axis_peer(stride, off) for stride in STRIDES for off in OTHERS]
    for peer in peers:
        pl.semaphore_signal(barrier, inc=1, device_id=peer, device_id_type=MESH)
    pl.semaphore_wait(barrier, len(peers))
    started = []

    def sender(src, dst, dev, waited=False):
        slot = len(started)
        copy = pltpu.make_async_remote_copy(src_ref=src, dst_ref=dst, send_sem=send_sem.at[slot], recv_sem=recv_sem.at[slot], device_id=dev, device_id_type=MESH)
        copy.start()
        started.append(None if waited else copy)
        return copy

    parts = range(s_width // PART)
    group_a = [PartSum(sender, credit.at[0, k], g_v, bufs_a, k, f_width, f_width + t_width) for k in parts]
    group_b = [PartSum(sender, credit.at[1, k], g_v, bufs_b, k, 0, f_width) for k in parts]
    small = SmallSum(sender, small_v, slots_v)

    def run(group, num):
        for part in group:
            getattr(part, STAGES[num])()

    small_v[0] = jnp.zeros(small_v.shape[1:], F32)
    for load in s_loads:
        load.wait()

    def state_of(b):
        n_seq = ROWS // half_len
        return s_v[pl.ds(b * n_seq, n_seq)].reshape(ROWS, s_width).astype(F32)

    def forward(b, carry):
        pltpu.make_async_copy(f_in.at[rows_of(b)], f_v.at[rows_of(b)], f_sem.at[b]).wait()
        state = state_of(b)
        target = jnp.dot(f_v[rows_of(b), :], sp_v[...], preferred_element_type=F32).astype(BF16)
        act = (rms_unit(state) * s_gain[...]).astype(BF16)
        act_v[rows_of(b), :] = act
        up_act, slope = gelu_pair(jnp.dot(act, su_v[...], preferred_element_type=F32))
        up_act = up_act.astype(BF16)
        slope_v[rows_of(b), :] = slope
        u_v[rows_of(b), :] = up_act
        new_state = (state + jnp.dot(up_act, sd_v[...], preferred_element_type=F32)).astype(BF16).astype(F32)
        error = target.astype(F32) - rms_unit(new_state)
        small_v[0, 1:2, 0:s_width] += jnp.sum(error * error, axis=0, keepdims=True)
        e_v[rows_of(b), :] = error.astype(BF16)
        d_v[rows_of(b), :] = rms_back(new_state, -grad_scale * error).astype(BF16)
        return carry

    def backward(b, carry):
        u_v[rows_of(b), :] = (slope_v[rows_of(b), :] * dot_cols(d_v[rows_of(b), :], sd_v[...])).astype(BF16)
        return carry

    def gain_sum(b, carry):
        d_act = dot_cols(u_v[rows_of(b), :], su_v[...])
        small_v[0, 0:1, 0:s_width] += jnp.sum(d_act * rms_unit(state_of(b)), axis=0, keepdims=True)
        return carry

    lax.fori_loop(0, n_blk, forward, 0, unroll=2)
    g_v[:, 2 * f_width : 2 * f_width + t_width] = grad_scale * dot_rows(e_v[...], f_v[...])
    g_v[:, f_width : 2 * f_width] = dot_rows(d_v[...], u_v[...])
    run(group_a, 0)
    lax.fori_loop(0, n_blk, backward, 0, unroll=2)
    run(group_a, 1)
    g_v[:, 0:f_width] = dot_rows(act_v[...], u_v[...])
    run(group_b, 0)
    run(group_a, 2)
    lax.fori_loop(0, n_blk // 2, gain_sum, 0)
    run(group_b, 1)
    lax.fori_loop(n_blk // 2, n_blk, gain_sum, 0)
    small_v[0, 2:3, 0:PART] = jnp.broadcast_to(jnp.sum(small_v[0, 1:2, 0:s_width], axis=1, keepdims=True), (1, PART))
    small.send()
    stores = [pltpu.make_async_copy(g_v.at[:, pl.ds(col, out.shape[1])], out, o_sem.at[i]) for i, (col, out) in enumerate([(0, up_out), (f_width, down_out), (2 * f_width, proj_out)])]
    final = len(STAGES) - 1
    for num in range(2, len(STAGES)):
        run(group_b, num)
        if num == final:
            stores[0].start()
        if num < final:
            run(group_a, num + 1)
            if num + 1 == final:
                stores[1].start()
                stores[2].start()
        if small.level <= len(STRIDES):
            small.add()
            if small.level <= len(STRIDES):
                small.send()
            else:
                small_out[...] = small_v[small.level]
    for store in stores:
        store.wait()
    for copy in started:
        if copy is not None:
            copy.wait_send()


def sum_bufs(parts, n_cols):
    wide, vmem = n_cols // RING, pltpu.VMEM
    half, quarter = SIDE // 2, SIDE // RING
    shapes = [(SIDE, n_cols), (2, half, wide), (2, half, wide), (2, SIDE, wide), (SIDE, wide), (len(OTHERS), quarter, wide), (RING, quarter, wide)]
    return [vmem((parts,) + shape, F32) for shape in shapes]


def student_sums(feat, stud, stud_r, s_gain, s_up, s_down, s_proj, grad_scale):
    n_tok, width = feat.shape
    n_blk = n_tok // ROWS
    seqs, half_len, s_width = stud_r.shape
    f_width = s_up.shape[2]
    n_cols = 2 * f_width + width
    parts = s_width // PART
    dma = pltpu.SemaphoreType.DMA
    vmem = pltpu.VMEM
    v_act = vmem((n_tok, s_width), BF16)
    small = (8, s_width)
    n_copies = 200
    return pl.pallas_call(
        functools.partial(student_kernel, n_blk, grad_scale),
        out_shape=tuple(jax.ShapeDtypeStruct(shape, F32) for shape in ((s_width, f_width), (s_width, f_width), (s_width, width), small)),
        in_specs=any_specs(3) + [VM] + any_specs(3),
        out_specs=any_specs(3) + [VM],
        scratch_shapes=[
            vmem((n_tok, width), BF16), vmem((n_tok // half_len, half_len, s_width), BF16), vmem((s_width, f_width), BF16), vmem((f_width, s_width), BF16), vmem((width, s_width), BF16),
            vmem((n_tok, f_width), BF16), vmem((n_tok, f_width), F32), v_act, v_act, v_act, vmem((s_width, n_cols), F32), vmem((5,) + small, F32), vmem((4, 4) + small, F32)]
        + sum_bufs(parts, f_width + width) + sum_bufs(parts, f_width)
        + [dma((n_blk,)), dma((5,)), dma((3,)), dma((n_copies,)), dma((n_copies,)), pltpu.SemaphoreType.REGULAR((2, parts))],
        compiler_params=pltpu.CompilerParams(collective_id=2, has_side_effects=True, vmem_limit_bytes=VMEM_MAX),
        cost_estimate=pl.CostEstimate(flops=2**34, bytes_accessed=2**24, transcendentals=0),
        name="student_sums",
    )(feat, stud, stud_r, s_gain, s_up, s_down, s_proj)


def unpack_kernel(inv_total, up_in, down_in, proj_in, small, up_out, down_out, proj_out, gain_out, loss_out):
    up_out[0] = up_in[...]
    down_out[0] = down_in[...].T
    proj_out[0] = proj_in[...].T
    gain_out[...] = small[0:1, :]
    loss_out[...] = small[2:3, 0:1] * inv_total


def unpack(grads_up, grads_down, grads_proj, small, total):
    rows, cols = grads_up.shape
    width = grads_proj.shape[1]
    steps = 2
    col, wid = cols // steps, width // steps

    def block(shape, index):
        return pl.BlockSpec(shape, index)

    return pl.pallas_call(
        functools.partial(unpack_kernel, 1.0 / total),
        grid=(steps,),
        out_shape=tuple(jax.ShapeDtypeStruct(shape, F32) for shape in ((1, rows, cols), (1, cols, rows), (1, width, rows), (1, rows), (1, 1))),
        in_specs=[block((rows, col), lambda i: (0, i)), block((rows, col), lambda i: (0, i)), block((rows, wid), lambda i: (0, i)), block(small.shape, lambda i: (0, 0))],
        out_specs=(block((1, rows, col), lambda i: (0, 0, i)), block((1, col, rows), lambda i: (0, i, 0)), block((1, wid, rows), lambda i: (0, i, 0)), block((1, rows), lambda i: (0, 0)), block((1, 1), lambda i: (0, 0))),
        compiler_params=pltpu.CompilerParams(vmem_limit_bytes=VMEM_MAX),
        name="unpack",
    )(grads_up, grads_down, grads_proj, small)


def solution(mesh):
    dev_count = mesh.shape["data"] * mesh.shape["model"]

    def body(teacher_in, student_in, teacher_gain, teacher_up, teacher_down, student_gain, student_up, student_down, student_proj):
        seq_rows, seq_len, s_width = student_in.shape
        total = seq_rows * dev_count * seq_len * s_width
        grad_scale = 2.0 / total
        t_width = teacher_in.shape[2]
        feat, stud_r = teacher(teacher_in.reshape(-1, t_width), teacher_gain, teacher_up, teacher_down, student_in)
        grad_up, grad_down, grad_proj, small = student_sums(feat, student_in, stud_r, student_gain, student_up, student_down, student_proj, grad_scale)
        grad_up, grad_down, grad_proj, grad_gain, loss = unpack(grad_up, grad_down, grad_proj, small, total)
        return (loss[0, 0], grad_up, grad_down, grad_gain, grad_proj)

    return jax.shard_map(
        body,
        mesh=mesh,
        in_specs=(
            P("data", "model", None),
            P(("data", "model"), None, None),
            P(),
            P(None, None, "model"),
            P(None, "model", None),
            P(),
            P(),
            P(),
            P(),
        ),
        out_specs=(P(), P(), P(), P(), P()),
        check_vma=False,
    )
```
